256 devices in a mesh: gx: 2 (over z_lo), gy: 16 (over x, y), gz: 8 (over z_hi, core).
Axes of the slice: x: 4, y: 4, z: 8 (z_hi: 4, z_lo: 2; z = z_hi * 2 + z_lo), core: 2. Of those that a mesh axis runs over, the one named last changes fastest.
Arguments:
- factors: bfloat16 [6144, 8, 4096], P('gy', None, 'gz'), may hold values from -0.046875 to 0.046875
- trial_vectors: float32 [64, 8, 4096], P('gx', None, 'gz'), may hold values from -6 to 6
- energy_gap: float32 [8, 4096], P(None, 'gz'), may hold values from 0.5 to 4
Outputs:
- updated_vectors: float32 [64, 8, 4096], P('gx', None, 'gz')
- coupling: float32 [64, 64], P(None, 'gx')
The draws below stay inside these ranges and needn't reach their ends.
All inputs are finite; a program needn't handle non-finite values.
Results may differ from the reference program's by a relative error of at most 0.02.
Values may be sent and summed in bfloat16 or wider, within the bound.
No kernel may reach another device: no remote copies, remote signals or barrier semaphores. Data moves between devices by JAX's collectives and lax.ppermute only.
A program may use at most 64 MiB of HBM per device.

```python
import math
import jax
import jax.numpy as jnp
from jax import lax

NBAS = 4096
NAUX = 6144
ROWS = 8
ITERS = 2
VECS = 64
N_GZ = 8


def draw_trial_vectors(key, part):
    first_key = jax.random.fold_in(jax.random.fold_in(key, 17), 0)
    base_draw = jnp.clip(jax.random.normal(first_key, (VECS, ROWS, NBAS), jnp.float32), -4.0, 4.0)
    return base_draw


def shard_levels(own_key, dims, cuts, low, top_value):
    factor_of = 1.0
    for position, blocks in cuts:
        steps = jax.random.uniform(jax.random.fold_in(jax.random.fold_in(own_key, 6), position), (blocks,), jnp.float32, low / len(cuts), top_value / len(cuts))
        factor_of = factor_of * jnp.repeat(jnp.exp(steps), dims[position] // blocks).reshape((-1,) + (1,) * (len(dims) - 1 - position))
    return factor_of


def centred(stream_key, dims, deviation, most, cuts=(), held_as=jnp.bfloat16):
    values = deviation * jax.random.normal(stream_key, dims, jnp.float32)
    if cuts:
        values = values * shard_levels(stream_key, dims, cuts, -0.22, 0.18)
    return jnp.clip(values, -most, most).astype(held_as)


def setup_inputs(seed: int = 0) -> dict:
    splits = jax.random.split(jax.random.key(seed), 4)
    return {
        "factors": centred(splits[0], (NAUX, ROWS, NBAS), (4 * NBAS) ** -0.5, 0.046875, ((0, 16), (2, 8))),
        "trial_vectors": draw_trial_vectors(jax.random.fold_in(splits[3], 71), 0),
        "energy_gap": jnp.clip(jnp.exp(math.log(4.0) - 2.0794415 * jax.random.uniform(splits[2], (ROWS, NBAS), jnp.float32) ** shard_levels(splits[2], (ROWS, NBAS), ((1, 8),), -0.2, 0.2)), 0.5, 4.0),
    }


def solve_subspace(gram_matrix, projected):
    lower_factor = jnp.linalg.cholesky(gram_matrix)
    inner_solve = lax.linalg.triangular_solve(lower_factor, projected, left_side=True, lower=True)
    return lax.linalg.triangular_solve(lower_factor, inner_solve, left_side=True, lower=True, transpose_a=True)

def reference(factors, trial_vectors, energy_gap):
    highest = lax.Precision.HIGHEST
    block_width = NBAS // N_GZ
    current = trial_vectors
    coupling = jnp.zeros((VECS, VECS), jnp.float32)
    for iteration in range(ITERS):
        compact = lax.optimization_barrier(current.astype(jnp.bfloat16)).astype(jnp.float32)
        fitted = jnp.zeros((VECS, NAUX), jnp.float32)
        mixed_fit = jnp.zeros((VECS, ROWS, ROWS, NAUX), jnp.float32)
        for column_block in range(N_GZ):
            start = column_block * block_width
            factor_block = factors[:, :, start:start + block_width].astype(jnp.float32)
            compact_block = compact[:, :, start:start + block_width]
            fitted = fitted + jnp.einsum('prn,krn->kp', factor_block, compact_block, precision=highest)
            partial_block = jnp.einsum('prn,kln->klrp', factor_block, compact_block, precision=highest)
            mixed_fit = mixed_fit + lax.optimization_barrier(partial_block.astype(jnp.bfloat16)).astype(jnp.float32)
        fitted_b = lax.optimization_barrier(fitted.astype(jnp.bfloat16)).astype(jnp.float32)
        mixed_b = lax.optimization_barrier(mixed_fit.astype(jnp.bfloat16)).astype(jnp.float32)
        pieces = []
        for column_block in range(N_GZ):
            start = column_block * block_width
            factor_block = factors[:, :, start:start + block_width].astype(jnp.float32)
            coulomb = jnp.einsum('prn,kp->krn', factor_block, fitted_b, precision=highest)
            exchange_part = jnp.einsum('klrp,pln->krn', mixed_b, factor_block, precision=highest)
            pieces.append(2.0 * coulomb - exchange_part)
        fock_part = jnp.concatenate(pieces, axis=2)
        sigma_all = energy_gap[None, :, :] * current + fock_part
        gram_matrix = jnp.einsum('krn,lrn->kl', current, current, precision=highest)
        projected = jnp.einsum('lrn,krn->lk', current, sigma_all, precision=highest)
        coupling = solve_subspace(gram_matrix, projected)
        residual = sigma_all - jnp.einsum('lrn,lk->krn', current, coupling, precision=highest)
        current = current - residual / energy_gap[None, :, :]
    return (current, coupling)
```

```python
import jax
import jax.numpy as jnp
from jax import lax
from jax.experimental import pallas as pl
from jax.experimental.pallas import tpu as pltpu
from jax.sharding import PartitionSpec as P

ITERS = 2
BF = jnp.bfloat16
F32 = jnp.float32
HIGHEST = lax.Precision.HIGHEST


NT = (((1,), (1,)), ((), ()))
NN = (((1,), (0,)), ((), ()))
TN = (((0,), (0,)), ((), ()))


def dot(a, b, dims, precision=None):
    return lax.dot_general(a, b, dims, precision=precision, preferred_element_type=F32)


SMEM = pl.BlockSpec(memory_space=pltpu.SMEM)
VMEM = pl.BlockSpec(memory_space=pltpu.VMEM)


def mix_kernel(order, x, b, out):
    rows, width = x.shape[1], b.shape[1]
    chosen = jnp.concatenate([x[order[j]] for j in range(4)], axis=0)
    for r in range(b.shape[0]):
        part = dot(chosen, b[r], NT).reshape(4, rows, width)
        out[:, r * rows : (r + 1) * rows, :] = part.astype(out.dtype)


def mix(order, x, b, dtype):
    r, k, _ = x.shape
    return pl.pallas_call(
        mix_kernel,
        out_shape=jax.ShapeDtypeStruct((4, r * k, b.shape[1]), dtype),
        in_specs=[SMEM, VMEM, VMEM],
        out_specs=VMEM,
    )(order, x, b)


def gram_kernel(own, other, gap, out):
    r, k, _ = own.shape
    gram = jnp.zeros((2 * k, 2 * k), F32)
    scaled = jnp.zeros((2 * k, k), F32)
    for i in range(r):
        both = jnp.concatenate([own[i], other[i]], axis=0)
        gram += dot(both, both, NT)
        mine = own[i].astype(F32) * gap[i : i + 1, :]
        high = mine.astype(BF)
        low = (mine - high.astype(F32)).astype(BF)
        scaled += dot(both, high, NT) + dot(both, low, NT)
    out[...] = jnp.concatenate([gram, scaled], axis=1)


def gram_parts(own, other, gap):
    k = own.shape[1]
    return pl.pallas_call(
        gram_kernel,
        out_shape=jax.ShapeDtypeStruct((2 * k, 3 * k), F32),
        in_specs=[VMEM] * 3,
        out_specs=VMEM,
    )(own, other, gap)


def fock_kernel(order, *refs):
    blocks = refs[:8]
    b, own, other, gram, out, message, coulomb = refs[8:]
    r, k, _ = own.shape
    fitted = jnp.zeros((k, b.shape[1]), F32)
    for j in range(8):
        start = pl.multiple_of(order[j] * k, k)
        fitted += blocks[j][pl.ds(start, k), :].astype(F32)
    fitted = fitted.astype(BF)
    total = jnp.zeros((r * k, b.shape[2]), F32)
    for j in range(8):
        both = dot(jnp.concatenate([blocks[j][...], fitted], axis=0), b[order[j]], NN)
        total += both[: r * k]
        coulomb[order[j]] = both[r * k :]
    projected = jnp.zeros((2 * k, k), F32)
    for i in range(r):
        part = 2.0 * coulomb[i] - total[i * k : (i + 1) * k]
        part = part.astype(BF)
        out[i * k : (i + 1) * k, :] = part
        projected += dot(jnp.concatenate([own[i], other[i]], axis=0), part, NT)
    message[...] = jnp.concatenate([gram[...], projected], axis=1)


def fock_parts(order, blocks, b, own, other, gram):
    r, k, n = own.shape
    return pl.pallas_call(
        fock_kernel,
        out_shape=(
            jax.ShapeDtypeStruct((r * k, n), BF),
            jax.ShapeDtypeStruct((2 * k, 4 * k), F32),
        ),
        in_specs=[SMEM] + [VMEM] * 12,
        out_specs=(VMEM, VMEM),
        scratch_shapes=[pltpu.VMEM((r, k, n), F32)],
    )(order, *blocks, b, own, other, gram)


def owner_kernel(arrived, sums, out, totals):
    total = sums[0]
    for j in range(1, sums.shape[0]):
        total += sums[j]
    totals[...] = total
    k = total.shape[1] // 4
    mine = total[:, 3 * k :]
    high = mine.astype(BF).astype(F32)
    low = mine - high
    tail = jnp.concatenate([high[:k], low[:k], high[k:], low[k:]], axis=1).astype(BF)
    fock = arrived[0].astype(F32)
    for j in range(1, arrived.shape[0]):
        fock += arrived[j].astype(F32)
    fock = fock.astype(BF)
    rows = fock.shape[0]
    for p in range(out.shape[0]):
        for i in range(4):
            out[p, i * rows : (i + 1) * rows, :] = fock[:, i * 128 : (i + 1) * 128]
        out[p, 4 * rows :, :] = tail


def owner_sums(arrived, sums):
    peers, rows, _ = arrived.shape
    k = sums.shape[2] // 4
    return pl.pallas_call(
        owner_kernel,
        out_shape=(
            jax.ShapeDtypeStruct((peers, 4 * rows + k, 128), BF),
            jax.ShapeDtypeStruct(sums.shape[1:], F32),
        ),
        in_specs=[VMEM, VMEM],
        out_specs=(VMEM, VMEM),
    )(arrived, sums)


def update_kernel(pieces, totals, inverse, own, other, gap, out, coupling):
    r, k, _ = own.shape
    peers = pieces.shape[0]
    rows = (pieces.shape[1] - k) // 4
    tail = pieces[0, 4 * rows :, :].astype(F32)
    for j in range(1, peers):
        tail += pieces[j, 4 * rows :, :].astype(F32)
    top = tail[:, :k] + tail[:, k : 2 * k]
    bottom = tail[:, 2 * k : 3 * k] + tail[:, 3 * k :]
    projected = totals[:, 2 * k : 3 * k] + jnp.concatenate([top, bottom], axis=0)
    inner = dot(inverse[...], projected, NN, HIGHEST)
    solved = dot(inverse[...], inner, TN, HIGHEST)
    coupling[...] = solved
    high = solved.astype(BF)
    low = (solved - high.astype(F32)).astype(BF)
    per_row = k // rows
    for i in range(r):
        both = jnp.concatenate([own[i], other[i]], axis=0)
        mixed = dot(high, both, TN) + dot(low, both, TN)
        fock = jnp.concatenate(
            [
                jnp.concatenate(
                    [
                        pieces[i * per_row + h, q * rows : (q + 1) * rows, :]
                        for q in range(4)
                    ],
                    axis=1,
                )
                for h in range(per_row)
            ],
            axis=0,
        )
        out[i] = ((mixed - fock.astype(F32)) / gap[i : i + 1, :]).astype(out.dtype)


def update(pieces, totals, inverse, own, other, gap, dtype):
    r, k, n = own.shape
    return pl.pallas_call(
        update_kernel,
        out_shape=(
            jax.ShapeDtypeStruct((r, k, n), dtype),
            jax.ShapeDtypeStruct((2 * k, k), F32),
        ),
        in_specs=[VMEM] * 6,
        out_specs=(VMEM, VMEM),
    )(pieces, totals, inverse, own, other, gap)


def inverse_factor(gram):
    lower = jnp.linalg.cholesky(gram)
    return lax.linalg.triangular_solve(
        lower, jnp.eye(gram.shape[0], dtype=F32), left_side=True, lower=True
    )


def ring(step):
    pairs = []
    for h in range(4):
        for c in range(2):
            way = step if c == 1 else -step
            pairs.append((2 * h + c, 2 * ((h + way) % 4) + c))
    return pairs


AHEAD = ring(1)
BACK = ring(-1)
SIBLING = [(i, i ^ 1) for i in range(8)]
OTHER = [(0, 1), (1, 0)]


def per_device(factors, trial_vectors, energy_gap):
    place = lax.axis_index("gz")
    high, core = place // 2, place % 2
    way = 2 * core - 1

    def rows_of(steps, c, direction):
        return [2 * ((high + s * direction) % 4) + c for s in steps]

    own_rows = jnp.stack(rows_of((2, 1, -1, 0), core, way)).astype(jnp.int32)
    sib_rows = jnp.stack(rows_of((2, 1, -1, 0), 1 - core, -way)).astype(jnp.int32)
    arrival = jnp.stack(
        rows_of((0, -1, 1, 2), core, way) + rows_of((0, -1, 1, 2), 1 - core, -way)
    ).astype(jnp.int32)

    b = jnp.transpose(factors, (1, 0, 2))
    current = jnp.transpose(trial_vectors, (1, 0, 2)).astype(BF)
    coupling = None

    def add(u, v):
        return (u.astype(F32) + v.astype(F32)).astype(BF)

    for iteration in range(ITERS):
        other = lax.ppermute(current, "gx", OTHER)
        theirs = mix(sib_rows, current, b, BF)
        theirs = lax.ppermute(theirs, "gz", SIBLING)
        mine = mix(own_rows, current, b, F32)
        far = lax.ppermute(add(mine[0], theirs[0]), "gz", AHEAD)
        near = lax.ppermute(add(mine[2], theirs[2]), "gz", BACK)
        far = lax.ppermute(
            (mine[1] + theirs[1].astype(F32) + far.astype(F32)).astype(BF), "gz", AHEAD
        )
        total = mine[3] + theirs[3].astype(F32) + near.astype(F32) + far.astype(F32)
        first = total.astype(BF)
        second = lax.ppermute(first, "gz", AHEAD)
        third = lax.ppermute(first, "gz", BACK)
        fourth = lax.ppermute(second, "gz", AHEAD)
        blocks = [first, second, third, fourth]
        blocks += [lax.ppermute(a, "gz", SIBLING) for a in blocks]
        gram = gram_parts(current, other, energy_gap)
        fock, sums = fock_parts(arrival, blocks, b, current, other, gram)
        sums = lax.all_to_all(
            jnp.broadcast_to(sums[None], (8, *sums.shape)), "gz", 0, 0, tiled=True
        )
        arrived = lax.all_to_all(fock.reshape(16, -1, fock.shape[1]), "gy", 0, 0, tiled=True)
        pieces, totals = owner_sums(arrived, sums)
        pieces = lax.all_to_all(pieces, "gy", 0, 0, tiled=True)
        inverse = inverse_factor(totals[:, : totals.shape[0]])
        last = iteration == ITERS - 1
        current, coupling = update(
            pieces, totals, inverse, current, other, energy_gap, F32 if last else BF
        )
    half = coupling.shape[0] // 2
    swapped = jnp.concatenate([coupling[half:], coupling[:half]], axis=0)
    coupling = jnp.where(lax.axis_index("gx") == 0, coupling, swapped)
    return (jnp.transpose(current, (1, 0, 2)), coupling)


def solution(mesh):
    placed = (P("gy", None, "gz"), P("gx", None, "gz"), P(None, "gz"))
    return jax.shard_map(
        per_device,
        mesh=mesh,
        in_specs=placed,
        out_specs=(P("gx", None, "gz"), P(None, "gx")),
        check_vma=False,
    )
```

```python
import jax
import jax.numpy as jnp
import numpy as np
from jax import lax
from jax.experimental import pallas as pl
from jax.experimental.pallas import tpu as pltpu
from jax.sharding import PartitionSpec as P

ITERS = 2
BF = jnp.bfloat16
F32 = jnp.float32
HIGHEST = lax.Precision.HIGHEST


NT = (((1,), (1,)), ((), ()))
NN = (((1,), (0,)), ((), ()))
TN = (((0,), (0,)), ((), ()))


def dot(a, b, dims, precision=None):
    return lax.dot_general(a, b, dims, precision=precision, preferred_element_type=F32)


SMEM = pl.BlockSpec(memory_space=pltpu.SMEM)
VMEM = pl.BlockSpec(memory_space=pltpu.VMEM)
PARAMS = pltpu.CompilerParams(vmem_limit_bytes=24 << 20)


def array(shape, dtype):
    return jax.ShapeDtypeStruct(shape, dtype)


def split(value):
    high = value.astype(BF).astype(F32)
    return high, value - high


def lanes(value, parts):
    rows = value.shape[0] // parts
    return jnp.concatenate([value[i * rows : (i + 1) * rows] for i in range(parts)], axis=1)


def unlanes(value, parts):
    width = value.shape[1] // parts
    return jnp.concatenate([value[:, i * width : (i + 1) * width] for i in range(parts)], axis=0)


def mix_kernel(order, x, b, *outs, first):
    rows = x.shape[1]
    chosen = jnp.concatenate([x[order[first + j]] for j in range(4)], axis=0)
    for r in range(b.shape[0]):
        part = dot(chosen, b[r], NT)
        for j in range(4):
            value = part[j * rows : (j + 1) * rows].astype(outs[0].dtype)
            if len(outs) == 1:
                outs[0][j, r * rows : (r + 1) * rows, :] = value
            else:
                outs[j][r * rows : (r + 1) * rows, :] = value


def mix(order, x, b, first, dtype, apart):
    r, k, _ = x.shape
    shape = (r * k, b.shape[1])
    outs = [array(shape, dtype)] * 4 if apart else [array((4, *shape), dtype)]
    return pl.pallas_call(
        lambda *refs: mix_kernel(*refs, first=first),
        out_shape=outs,
        in_specs=[SMEM, VMEM, VMEM],
        out_specs=[VMEM] * len(outs),
        compiler_params=PARAMS,
    )(order, x, b)


def gram_kernel(own, other, gap, out):
    r, k, _ = own.shape
    gram = jnp.zeros((2 * k, 2 * k), F32)
    scaled = jnp.zeros((2 * k, k), F32)
    for i in range(r):
        both = jnp.concatenate([own[i], other[i]], axis=0)
        gram += dot(both, both, NT)
        mine = own[i].astype(F32) * gap[i : i + 1, :]
        high, low = split(mine)
        scaled += dot(both, high.astype(BF), NT) + dot(both, low.astype(BF), NT)
    high, low = split(lanes(gram, 2))
    scaled_high, scaled_low = split(lanes(scaled, 2))
    out[...] = jnp.concatenate([high, low, scaled_high, scaled_low], axis=1).astype(BF)


def gram_parts(own, other, gap):
    k = own.shape[1]
    return pl.pallas_call(
        gram_kernel,
        out_shape=array((k, 12 * k), BF),
        in_specs=[VMEM] * 3,
        out_specs=VMEM,
        compiler_params=PARAMS,
    )(own, other, gap)


def total_kernel(mine, theirs, near, far, tail, out):
    rows = mine.shape[0]
    total = mine[...] + theirs[0].astype(F32) + near[...].astype(F32) + far[...].astype(F32)
    out[:rows, :] = total.astype(BF)
    out[rows:, :] = tail[...]


def total_block(mine, theirs, near, far, tail):
    rows, width = mine.shape
    whole = pl.BlockSpec((rows, width), lambda i: (0, 0))
    return pl.pallas_call(
        total_kernel,
        grid=(1,),
        out_shape=array((rows + tail.shape[0], width), BF),
        in_specs=[
            whole,
            pl.BlockSpec((1, rows, width), lambda i: (3, 0, 0)),
            whole,
            whole,
            pl.BlockSpec(tail.shape, lambda i: (0, 0)),
        ],
        out_specs=pl.BlockSpec((rows + tail.shape[0], width), lambda i: (0, 0)),
        compiler_params=PARAMS,
    )(mine, theirs, near, far, tail)


def fock_kernel(order, *refs):
    blocks = refs[:8]
    b, own, other, out, gram, scaled, message, coulomb = refs[8:]
    r, k, _ = own.shape
    rows = r * k
    fitted = jnp.zeros((k, b.shape[1]), F32)
    tail = jnp.zeros((blocks[0].shape[0] - rows, b.shape[1]), F32)
    for j in range(8):
        start = pl.multiple_of(order[8 + j] * k, k)
        fitted += blocks[j][pl.ds(start, k), :].astype(F32)
        tail += blocks[j][rows:, :].astype(F32)
    gram[...] = unlanes(tail[:, : 4 * k] + tail[:, 4 * k : 8 * k], 2)
    scaled[...] = unlanes(tail[:, 8 * k : 10 * k] + tail[:, 10 * k :], 2)
    fitted = fitted.astype(BF)
    total = jnp.zeros((rows, b.shape[2]), F32)
    for j in range(8):
        place = order[8 + j]
        both = dot(jnp.concatenate([blocks[j][:rows, :], fitted], axis=0), b[place], NN)
        total += both[:rows]
        coulomb[place] = both[rows:]
    projected = jnp.zeros((2 * k, k), F32)
    for i in range(r):
        part = 2.0 * coulomb[i] - total[i * k : (i + 1) * k]
        part = part.astype(BF)
        out[i * k : (i + 1) * k, :] = part
        projected += dot(jnp.concatenate([own[i], other[i]], axis=0), part, NT)
    message[...] = lanes(projected, 4)


def fock_parts(order, blocks, b, own, other):
    r, k, n = own.shape
    return pl.pallas_call(
        fock_kernel,
        out_shape=(
            array((r * k, n), BF),
            array((2 * k, 2 * k), F32),
            array((2 * k, k), F32),
            array((k // 2, 4 * k), F32),
        ),
        in_specs=[SMEM] + [VMEM] * 11,
        out_specs=(VMEM,) * 4,
        scratch_shapes=[pltpu.VMEM((r, k, n), F32)],
        compiler_params=PARAMS,
    )(order, *blocks, b, own, other)


def owner_kernel(arrived, projected, out):
    high, low = split(projected[...])
    tail = jnp.concatenate([high, low], axis=0).astype(BF)
    fock = arrived[0].astype(F32)
    for j in range(1, arrived.shape[0]):
        fock += arrived[j].astype(F32)
    fock = fock.astype(BF)
    rows = fock.shape[0]
    for p in range(out.shape[0]):
        for i in range(4):
            out[p, i * rows : (i + 1) * rows, :] = fock[:, i * 128 : (i + 1) * 128]
        out[p, 4 * rows :, :] = tail


def owner_sums(arrived, projected):
    peers, rows, _ = arrived.shape
    return pl.pallas_call(
        owner_kernel,
        out_shape=array((peers, 4 * rows + 2 * projected.shape[0], 128), BF),
        in_specs=[VMEM, VMEM],
        out_specs=VMEM,
        compiler_params=PARAMS,
    )(arrived, projected)


def update_kernel(pieces, scaled, inverse, own, other, gap, out, coupling):
    r, k, _ = own.shape
    peers = pieces.shape[0]
    rows = (pieces.shape[1] - k) // 4
    tail = pieces[0, 4 * rows :, :].astype(F32)
    for j in range(1, peers):
        tail += pieces[j, 4 * rows :, :].astype(F32)
    projected = scaled[...] + unlanes(tail[: k // 2] + tail[k // 2 :], 4)
    inner = dot(inverse[...], projected, NN, HIGHEST)
    solved = dot(inverse[...], inner, TN, HIGHEST)
    coupling[...] = solved
    high, low = split(solved)
    high, low = high.astype(BF), low.astype(BF)
    per_row = k // rows
    for i in range(r):
        both = jnp.concatenate([own[i], other[i]], axis=0)
        mixed = dot(high, both, TN) + dot(low, both, TN)
        fock = jnp.concatenate(
            [
                jnp.concatenate(
                    [
                        pieces[i * per_row + h, q * rows : (q + 1) * rows, :]
                        for q in range(4)
                    ],
                    axis=1,
                )
                for h in range(per_row)
            ],
            axis=0,
        )
        out[i] = ((mixed - fock.astype(F32)) / gap[i : i + 1, :]).astype(out.dtype)


def update(pieces, scaled, inverse, own, other, gap, dtype):
    r, k, n = own.shape
    return pl.pallas_call(
        update_kernel,
        out_shape=(array((r, k, n), dtype), array((2 * k, k), F32)),
        in_specs=[VMEM] * 6,
        out_specs=(VMEM, VMEM),
        compiler_params=PARAMS,
    )(pieces, scaled, inverse, own, other, gap)


def inverse_factor(gram):
    lower = jnp.linalg.cholesky(gram)
    return lax.linalg.triangular_solve(
        lower, jnp.eye(gram.shape[0], dtype=F32), left_side=True, lower=True
    )


def ring(step):
    pairs = []
    for h in range(4):
        for c in range(2):
            way = step if c == 1 else -step
            pairs.append((2 * h + c, 2 * ((h + way) % 4) + c))
    return pairs


AHEAD = ring(1)
BACK = ring(-1)
SIBLING = [(i, i ^ 1) for i in range(8)]
ACROSS = [(i, i ^ 2) for i in range(8)]
OPPOSITE = [(i, i ^ 4) for i in range(8)]
OTHER = [(0, 1), (1, 0)]


def row_table():
    table = np.zeros((8, 16), np.int32)
    for place in range(8):
        h, c = divmod(place, 2)

        def rows(steps, core):
            way = 2 * core - 1
            return [2 * ((h + s * way) % 4) + core for s in steps]

        sent, got = (2, 1, -1, 0), (0, -1, 1, 2)
        table[place] = (
            rows(sent, c) + rows(sent, 1 - c) + rows(got, c) + rows(got, 1 - c)
        )
    return table


def per_device(factors, trial_vectors, energy_gap):
    order = jnp.asarray(row_table())[lax.axis_index("gz")]
    current = jnp.transpose(trial_vectors, (1, 0, 2)).astype(BF)
    b = jnp.transpose(factors, (1, 0, 2))
    coupling = None

    def add(*terms):
        return sum(t.astype(F32) for t in terms).astype(BF)

    for iteration in range(ITERS):
        other = lax.ppermute(current, "gx", OTHER)
        (theirs,) = mix(order, current, b, 4, BF, False)
        theirs = lax.ppermute(theirs, "gz", SIBLING)
        mine = mix(order, current, b, 0, F32, True)
        tail = gram_parts(current, other, energy_gap)
        far = lax.ppermute(add(mine[0], theirs[0]), "gz", AHEAD)
        near = lax.ppermute(add(mine[2], theirs[2]), "gz", BACK)
        far = lax.ppermute(add(mine[1], theirs[1], far), "gz", AHEAD)
        first = total_block(mine[3], theirs, near, far, tail)
        second = lax.ppermute(first, "gz", AHEAD)
        third = lax.ppermute(first, "gz", BACK)
        fourth = lax.ppermute(second, "gz", AHEAD)
        blocks = [first, second, third, fourth]
        blocks += [lax.ppermute(a, "gz", SIBLING) for a in blocks]
        fock, gram, scaled, projected = fock_parts(order, blocks, b, current, other)
        arrived = lax.all_to_all(fock.reshape(16, -1, fock.shape[1]), "gy", 0, 0, tiled=True)
        inverse = inverse_factor(gram)
        for pairs in (SIBLING, ACROSS, OPPOSITE):
            projected = projected + lax.ppermute(projected, "gz", pairs)
        pieces = owner_sums(arrived, projected)
        pieces = lax.all_to_all(pieces, "gy", 0, 0, tiled=True)
        last = iteration == ITERS - 1
        current, coupling = update(
            pieces, scaled, inverse, current, other, energy_gap, F32 if last else BF
        )
    half = coupling.shape[0] // 2
    swapped = jnp.concatenate([coupling[half:], coupling[:half]], axis=0)
    coupling = jnp.where(lax.axis_index("gx") == 0, coupling, swapped)
    return (jnp.transpose(current, (1, 0, 2)), coupling)


def solution(mesh):
    placed = (P("gy", None, "gz"), P("gx", None, "gz"), P(None, "gz"))
    return jax.shard_map(
        per_device,
        mesh=mesh,
        in_specs=placed,
        out_specs=(P("gx", None, "gz"), P(None, "gx")),
        check_vma=False,
    )
```

```python
import jax
import jax.numpy as jnp
import numpy as np
from jax import lax
from jax.experimental import pallas as pl
from jax.experimental.pallas import tpu as pltpu
from jax.sharding import PartitionSpec as P

ITERS = 2
BF = jnp.bfloat16
F32 = jnp.float32
HIGHEST = lax.Precision.HIGHEST


NT = (((1,), (1,)), ((), ()))
NN = (((1,), (0,)), ((), ()))
TN = (((0,), (0,)), ((), ()))


def dot(a, b, dims, precision=None):
    return lax.dot_general(a, b, dims, precision=precision, preferred_element_type=F32)


SMEM = pl.BlockSpec(memory_space=pltpu.SMEM)
VMEM = pl.BlockSpec(memory_space=pltpu.VMEM)
PARAMS = pltpu.CompilerParams(vmem_limit_bytes=24 << 20)


def array(shape, dtype):
    return jax.ShapeDtypeStruct(shape, dtype)


def split(value):
    high = value.astype(BF).astype(F32)
    return high, value - high


def lanes(value, parts):
    rows = value.shape[0] // parts
    return jnp.concatenate([value[i * rows : (i + 1) * rows] for i in range(parts)], axis=1)


def unlanes(value, parts):
    width = value.shape[1] // parts
    return jnp.concatenate([value[:, i * width : (i + 1) * width] for i in range(parts)], axis=0)


def mix_kernel(order, x, b, *outs, first):
    rows = x.shape[1]
    chosen = jnp.concatenate([x[order[first + j]] for j in range(4)], axis=0)
    for r in range(b.shape[0]):
        part = dot(chosen, b[r], NT)
        for j in range(4):
            value = part[j * rows : (j + 1) * rows].astype(outs[0].dtype)
            if len(outs) == 1:
                outs[0][j, r * rows : (r + 1) * rows, :] = value
            else:
                outs[j][r * rows : (r + 1) * rows, :] = value


def mix(order, x, b, first, dtype, apart):
    r, k, _ = x.shape
    shape = (r * k, b.shape[1])
    outs = [array(shape, dtype)] * 4 if apart else [array((4, *shape), dtype)]
    return pl.pallas_call(
        lambda *refs: mix_kernel(*refs, first=first),
        out_shape=outs,
        in_specs=[SMEM, VMEM, VMEM],
        out_specs=[VMEM] * len(outs),
        compiler_params=PARAMS,
    )(order, x, b)


def gram_kernel(own, other, gap, out):
    r, k, _ = own.shape
    gram = jnp.zeros((2 * k, 2 * k), F32)
    scaled = jnp.zeros((2 * k, k), F32)
    for i in range(r):
        both = jnp.concatenate([own[i], other[i]], axis=0)
        gram += dot(both, both, NT)
        mine = own[i].astype(F32) * gap[i : i + 1, :]
        high, low = split(mine)
        scaled += dot(both, high.astype(BF), NT) + dot(both, low.astype(BF), NT)
    out[...] = jnp.concatenate([gram, scaled], axis=1)


def gram_parts(own, other, gap):
    k = own.shape[1]
    return pl.pallas_call(
        gram_kernel,
        out_shape=array((2 * k, 3 * k), F32),
        in_specs=[VMEM] * 3,
        out_specs=VMEM,
        compiler_params=PARAMS,
    )(own, other, gap)


def fock_kernel(order, *refs):
    blocks = refs[:8]
    b, own, other, gram, out, message, coulomb = refs[8:]
    r, k, _ = own.shape
    rows = r * k
    fitted = jnp.zeros((k, b.shape[1]), F32)
    for j in range(8):
        start = pl.multiple_of(order[8 + j] * k, k)
        fitted += blocks[j][pl.ds(start, k), :].astype(F32)
    fitted = fitted.astype(BF)
    total = jnp.zeros((rows, b.shape[2]), F32)
    for j in range(8):
        place = order[8 + j]
        both = dot(jnp.concatenate([blocks[j][...], fitted], axis=0), b[place], NN)
        total += both[:rows]
        coulomb[place] = both[rows:]
    projected = jnp.zeros((2 * k, k), F32)
    for i in range(r):
        part = 2.0 * coulomb[i] - total[i * k : (i + 1) * k]
        part = part.astype(BF)
        out[i * k : (i + 1) * k, :] = part
        projected += dot(jnp.concatenate([own[i], other[i]], axis=0), part, NT)
    message[...] = jnp.concatenate([gram[...], projected], axis=1)


def fock_parts(order, blocks, b, own, other, gram):
    r, k, n = own.shape
    return pl.pallas_call(
        fock_kernel,
        out_shape=(array((r * k, n), BF), array((2 * k, 4 * k), F32)),
        in_specs=[SMEM] + [VMEM] * 12,
        out_specs=(VMEM, VMEM),
        scratch_shapes=[pltpu.VMEM((r, k, n), F32)],
        compiler_params=PARAMS,
    )(order, *blocks, b, own, other, gram)


def owner_kernel(arrived, s0, s1, s2, s3, out, totals):
    total = (s0[...] + s1[...]) + (s2[...] + s3[...])
    totals[...] = total
    high, low = split(lanes(total[:, 3 * total.shape[1] // 4 :], 4))
    tail = jnp.concatenate([high, low], axis=0).astype(BF)
    fock = arrived[0].astype(F32)
    for j in range(1, arrived.shape[0]):
        fock += arrived[j].astype(F32)
    fock = fock.astype(BF)
    rows = fock.shape[0]
    for p in range(out.shape[0]):
        for i in range(4):
            out[p, i * rows : (i + 1) * rows, :] = fock[:, i * 128 : (i + 1) * 128]
        out[p, 4 * rows :, :] = tail


def owner_sums(arrived, sums):
    peers, rows, _ = arrived.shape
    shape = sums[0].shape
    return pl.pallas_call(
        owner_kernel,
        out_shape=(
            array((peers, 4 * rows + shape[0] // 2, 128), BF),
            array(shape, F32),
        ),
        in_specs=[VMEM] * 5,
        out_specs=(VMEM, VMEM),
        compiler_params=PARAMS,
    )(arrived, *sums)


def inverse_kernel(totals, out):
    size = totals.shape[0]
    rows = lax.broadcasted_iota(jnp.int32, (size, 2 * size), 0)
    columns = lax.broadcasted_iota(jnp.int32, (size, 2 * size), 1)
    identity = (columns == rows + size).astype(F32)
    work = jnp.where(columns < size, totals[...], identity)
    for j in range(0, size, 2):
        first, second = work[j : j + 1], work[j + 1 : j + 2]
        aa, ab, bb = first[:, j : j + 1], first[:, j + 1 : j + 2], second[:, j + 1 : j + 2]
        scale = 1.0 / (aa * bb - ab * ab)
        top = (bb * scale) * first - (ab * scale) * second
        bottom = (aa * scale) * second - (ab * scale) * first
        rest = work - work[:, j : j + 1] * top - work[:, j + 1 : j + 2] * bottom
        work = jnp.where(rows == j, top, jnp.where(rows == j + 1, bottom, rest))
    out[...] = work[:, size:]


def inverse_of(totals):
    size = totals.shape[0]
    return pl.pallas_call(
        inverse_kernel,
        out_shape=array((size, size), F32),
        in_specs=[VMEM],
        out_specs=VMEM,
        compiler_params=PARAMS,
    )(totals)


def update_kernel(pieces, totals, inverse, own, other, gap, out, coupling):
    r, k, _ = own.shape
    peers = pieces.shape[0]
    rows = (pieces.shape[1] - k) // 4
    tail = pieces[0, 4 * rows :, :].astype(F32)
    for j in range(1, peers):
        tail += pieces[j, 4 * rows :, :].astype(F32)
    projected = totals[:, 2 * k : 3 * k] + unlanes(tail[: k // 2] + tail[k // 2 :], 4)
    solved = dot(inverse[...], projected, NN, HIGHEST)
    coupling[...] = solved
    high, low = split(solved)
    high, low = high.astype(BF), low.astype(BF)
    per_row = k // rows
    for i in range(r):
        both = jnp.concatenate([own[i], other[i]], axis=0)
        mixed = dot(high, both, TN) + dot(low, both, TN)
        fock = jnp.concatenate(
            [
                jnp.concatenate(
                    [
                        pieces[i * per_row + h, q * rows : (q + 1) * rows, :]
                        for q in range(4)
                    ],
                    axis=1,
                )
                for h in range(per_row)
            ],
            axis=0,
        )
        out[i] = ((mixed - fock.astype(F32)) / gap[i : i + 1, :]).astype(out.dtype)


def update(pieces, totals, inverse, own, other, gap, dtype):
    r, k, n = own.shape
    return pl.pallas_call(
        update_kernel,
        out_shape=(array((r, k, n), dtype), array((2 * k, k), F32)),
        in_specs=[VMEM] * 6,
        out_specs=(VMEM, VMEM),
        compiler_params=PARAMS,
    )(pieces, totals, inverse, own, other, gap)


def ring(step):
    pairs = []
    for h in range(4):
        for c in range(2):
            way = step if c == 1 else -step
            pairs.append((2 * h + c, 2 * ((h + way) % 4) + c))
    return pairs


AHEAD = ring(1)
BACK = ring(-1)
SIBLING = [(i, i ^ 1) for i in range(8)]
OTHER = [(0, 1), (1, 0)]


def row_table():
    table = np.zeros((8, 16), np.int32)
    for place in range(8):
        h, c = divmod(place, 2)

        def rows(steps, core):
            way = 2 * core - 1
            return [2 * ((h + s * way) % 4) + core for s in steps]

        sent, got = (2, 1, -1, 0), (0, -1, 1, 2)
        table[place] = (
            rows(sent, c) + rows(sent, 1 - c) + rows(got, c) + rows(got, 1 - c)
        )
    return table


def per_device(factors, trial_vectors, energy_gap):
    order = jnp.asarray(row_table())[lax.axis_index("gz")]
    current = jnp.transpose(trial_vectors, (1, 0, 2)).astype(BF)
    b = jnp.transpose(factors, (1, 0, 2))
    coupling = None

    def add(*terms):
        return sum(t.astype(F32) for t in terms).astype(BF)

    for iteration in range(ITERS):
        other = lax.ppermute(current, "gx", OTHER)
        (theirs,) = mix(order, current, b, 4, BF, False)
        theirs = lax.ppermute(theirs, "gz", SIBLING)
        mine = mix(order, current, b, 0, F32, True)
        gram = gram_parts(current, other, energy_gap)
        far = lax.ppermute(add(mine[0], theirs[0]), "gz", AHEAD)
        near = lax.ppermute(add(mine[2], theirs[2]), "gz", BACK)
        far = lax.ppermute(add(mine[1], theirs[1], far), "gz", AHEAD)
        first = add(mine[3], theirs[3], near, far)
        second = lax.ppermute(first, "gz", AHEAD)
        third = lax.ppermute(first, "gz", BACK)
        fourth = lax.ppermute(second, "gz", AHEAD)
        blocks = [first, second, third, fourth]
        blocks += [lax.ppermute(a, "gz", SIBLING) for a in blocks]
        fock, sums = fock_parts(order, blocks, b, current, other, gram)
        arrived = lax.all_to_all(fock.reshape(16, -1, fock.shape[1]), "gy", 0, 0, tiled=True)
        sums = sums + lax.ppermute(sums, "gz", SIBLING)
        sums = [sums] + [
            lax.ppermute(sums, "gz", [(i, i ^ flip) for i in range(8)]) for flip in (2, 4, 6)
        ]
        pieces, totals = owner_sums(arrived, sums)
        pieces = lax.all_to_all(pieces, "gy", 0, 0, tiled=True)
        inverse = inverse_of(totals)
        last = iteration == ITERS - 1
        current, coupling = update(
            pieces, totals, inverse, current, other, energy_gap, F32 if last else BF
        )
    half = coupling.shape[0] // 2
    swapped = jnp.concatenate([coupling[half:], coupling[:half]], axis=0)
    coupling = jnp.where(lax.axis_index("gx") == 0, coupling, swapped)
    return (jnp.transpose(current, (1, 0, 2)), coupling)


def solution(mesh):
    placed = (P("gy", None, "gz"), P("gx", None, "gz"), P(None, "gz"))
    return jax.shard_map(
        per_device,
        mesh=mesh,
        in_specs=placed,
        out_specs=(P("gx", None, "gz"), P(None, "gx")),
        check_vma=False,
    )
```

```python
import jax
import jax.numpy as jnp
from jax import lax
from jax.experimental import pallas as pl
from jax.experimental.pallas import tpu as pltpu
from jax.sharding import PartitionSpec as P

ITERS = 2
BF = jnp.bfloat16
F32 = jnp.float32
HIGHEST = lax.Precision.HIGHEST


NT = (((1,), (1,)), ((), ()))
NN = (((1,), (0,)), ((), ()))
TN = (((0,), (0,)), ((), ()))


def dot(a, b, dims, precision=None):
    return lax.dot_general(a, b, dims, precision=precision, preferred_element_type=F32)


SMEM = pl.BlockSpec(memory_space=pltpu.SMEM)
VMEM = pl.BlockSpec(memory_space=pltpu.VMEM)
PARAMS = pltpu.CompilerParams(vmem_limit_bytes=24 << 20)


def array(shape, dtype):
    return jax.ShapeDtypeStruct(shape, dtype)


def split(value):
    high = value.astype(BF).astype(F32)
    return high, value - high


def lanes(value, parts):
    rows = value.shape[0] // parts
    return jnp.concatenate([value[i * rows : (i + 1) * rows] for i in range(parts)], axis=1)


def unlanes(value, parts):
    width = value.shape[1] // parts
    return jnp.concatenate([value[:, i * width : (i + 1) * width] for i in range(parts)], axis=0)


def rows_of(steps, place, sibling):
    chip = place >> 1
    core = (1 - (place & 1)) if sibling else (place & 1)
    way = 2 * core - 1
    return [2 * ((chip + s * way) & 3) + core for s in steps]


def mix_kernel(place, x, b, *outs, sibling):
    rows = x.shape[1]
    order = rows_of((2, 1, -1, 0), place[2], sibling)
    chosen = jnp.concatenate([x[j] for j in order], axis=0)
    for r in range(b.shape[0]):
        part = dot(chosen, b[r], NT)
        for j in range(4):
            value = part[j * rows : (j + 1) * rows].astype(outs[0].dtype)
            if len(outs) == 1:
                outs[0][j, r * rows : (r + 1) * rows, :] = value
            else:
                outs[j][r * rows : (r + 1) * rows, :] = value


def mix(place, x, b, sibling, dtype, apart):
    r, k, _ = x.shape
    shape = (r * k, b.shape[1])
    outs = [array(shape, dtype)] * 4 if apart else [array((4, *shape), dtype)]
    return pl.pallas_call(
        lambda *refs: mix_kernel(*refs, sibling=sibling),
        out_shape=outs,
        in_specs=[SMEM, VMEM, VMEM],
        out_specs=[VMEM] * len(outs),
        compiler_params=PARAMS,
    )(place, x, b)


def gram_kernel(own, other, gap, out):
    r, k, _ = own.shape
    gram = jnp.zeros((2 * k, 2 * k), F32)
    scaled = jnp.zeros((2 * k, k), F32)
    for i in range(r):
        both = jnp.concatenate([own[i], other[i]], axis=0)
        gram += dot(both, both, NT)
        mine = own[i].astype(F32) * gap[i : i + 1, :]
        high, low = split(mine)
        scaled += dot(both, high.astype(BF), NT) + dot(both, low.astype(BF), NT)
    out[...] = jnp.concatenate([gram, scaled], axis=1)


def gram_parts(own, other, gap):
    k = own.shape[1]
    return pl.pallas_call(
        gram_kernel,
        out_shape=array((2 * k, 3 * k), F32),
        in_specs=[VMEM] * 3,
        out_specs=VMEM,
        compiler_params=PARAMS,
    )(own, other, gap)


def fock_kernel(place, *refs):
    blocks = refs[:8]
    b, own, other, gram, out, message, coulomb = refs[8:]
    r, k, _ = own.shape
    rows = r * k
    got = (0, -1, 1, 2)
    order = rows_of(got, place[2], False) + rows_of(got, place[2], True)
    fitted = jnp.zeros((k, b.shape[1]), F32)
    for j in range(8):
        start = pl.multiple_of(order[j] * k, k)
        fitted += blocks[j][pl.ds(start, k), :].astype(F32)
    fitted = fitted.astype(BF)
    total = jnp.zeros((rows, b.shape[2]), F32)
    for j in range(8):
        both = dot(jnp.concatenate([blocks[j][...], fitted], axis=0), b[order[j]], NN)
        total += both[:rows]
        coulomb[order[j]] = both[rows:]
    projected = jnp.zeros((2 * k, k), F32)
    for i in range(r):
        part = 2.0 * coulomb[i] - total[i * k : (i + 1) * k]
        part = part.astype(BF)
        out[i * k : (i + 1) * k, :] = part
        projected += dot(jnp.concatenate([own[i], other[i]], axis=0), part, NT)
    once = jnp.where(place[1] == 0, 1.0, 0.0)
    projected += once * gram[:, 2 * k :]
    message[...] = jnp.concatenate([lanes(gram[:, : 2 * k], 2), lanes(projected, 4)], axis=0)


def fock_parts(place, blocks, b, own, other, gram):
    r, k, n = own.shape
    return pl.pallas_call(
        fock_kernel,
        out_shape=(array((r * k, n), BF), array((3 * k // 2, 4 * k), F32)),
        in_specs=[SMEM] + [VMEM] * 12,
        out_specs=(VMEM, VMEM),
        scratch_shapes=[pltpu.VMEM((r, k, n), F32)],
        compiler_params=PARAMS,
    )(place, *blocks, b, own, other, gram)


def owner_kernel(arrived, s0, s1, s2, s3, out, totals):
    total = (s0[...] + s1[...]) + (s2[...] + s3[...])
    size = totals.shape[0]
    totals[...] = total[:size]
    high, low = split(total[size:])
    tail = jnp.concatenate([high, low], axis=0).astype(BF)
    fock = arrived[0].astype(F32)
    for j in range(1, arrived.shape[0]):
        fock += arrived[j].astype(F32)
    fock = fock.astype(BF)
    rows = fock.shape[0]
    for p in range(out.shape[0]):
        for i in range(4):
            out[p, i * rows : (i + 1) * rows, :] = fock[:, i * 128 : (i + 1) * 128]
        out[p, 4 * rows :, :] = tail


def owner_sums(arrived, sums, copies):
    rows = arrived.shape[1]
    k = 2 * sums[0].shape[0] // 3
    return pl.pallas_call(
        owner_kernel,
        out_shape=(array((copies, 4 * rows + k, 128), BF), array((k, 128), F32)),
        in_specs=[VMEM] * 5,
        out_specs=(VMEM, VMEM),
        compiler_params=PARAMS,
    )(arrived, *sums)


def inverse_kernel(totals, out):
    size = 2 * totals.shape[0]
    half = unlanes(totals[...], 2)
    rows = lax.broadcasted_iota(jnp.int32, (size, 2 * size), 0)
    columns = lax.broadcasted_iota(jnp.int32, (size, 2 * size), 1)
    identity = (columns == rows + size).astype(F32)
    work = jnp.concatenate([half, identity[:, size:]], axis=1)
    for j in range(0, size, 2):
        first, second = work[j : j + 1], work[j + 1 : j + 2]
        aa, ab, bb = first[:, j : j + 1], first[:, j + 1 : j + 2], second[:, j + 1 : j + 2]
        scale = 1.0 / (aa * bb - ab * ab)
        top = (bb * scale) * first - (ab * scale) * second
        bottom = (aa * scale) * second - (ab * scale) * first
        rest = work - work[:, j : j + 1] * top - work[:, j + 1 : j + 2] * bottom
        work = jnp.where(rows == j, top, jnp.where(rows == j + 1, bottom, rest))
    out[...] = work[:, size:]


def inverse_of(totals):
    size = 2 * totals.shape[0]
    return pl.pallas_call(
        inverse_kernel,
        out_shape=array((size, size), F32),
        in_specs=[VMEM],
        out_specs=VMEM,
        compiler_params=PARAMS,
    )(totals)


def solve(pieces, base, inverse, k, rows, swap=False):
    tail = jnp.zeros((k, 4 * k), F32)
    for j in range(16):
        tail += pieces[base + j, 4 * rows :, :].astype(F32)
    projected = unlanes(tail[: k // 2] + tail[k // 2 :], 4)
    if swap:
        projected = jnp.concatenate([projected[k:], projected[:k]], axis=0)
    return dot(inverse[...], projected, NN, HIGHEST)


def fock_rows(pieces, base, i, k, rows):
    per_row = k // rows
    parts = []
    for h in range(per_row):
        piece = pieces[base + i * per_row + h, : 4 * rows, :]
        parts.append(lanes(piece, 4))
    return jnp.concatenate(parts, axis=0).astype(F32)


def step_kernel(place, pieces, inverse, own, other, gap, own_out, other_out):
    r, k, _ = own.shape
    rows = (pieces.shape[1] - k) // 4
    bases = [16 * place[0], 16 * (1 - place[0])]
    mine = solve(pieces, bases[0], inverse, k, rows)
    theirs = solve(pieces, bases[1], inverse, k, rows, swap=True)
    high, low = split(jnp.concatenate([mine, theirs], axis=1))
    high, low = high.astype(BF), low.astype(BF)
    for i in range(r):
        both = jnp.concatenate([own[i], other[i]], axis=0)
        mixed = dot(high, both, TN) + dot(low, both, TN)
        inverse_gap = 1.0 / gap[i : i + 1, :]
        for out, base, part in zip((own_out, other_out), bases, (mixed[:k], mixed[k:])):
            out[i] = ((part - fock_rows(pieces, base, i, k, rows)) * inverse_gap).astype(BF)


def step_update(place, pieces, inverse, own, other, gap):
    return pl.pallas_call(
        step_kernel,
        out_shape=(array(own.shape, BF), array(own.shape, BF)),
        in_specs=[SMEM] + [VMEM] * 5,
        out_specs=(VMEM, VMEM),
        compiler_params=PARAMS,
    )(place, pieces, inverse, own, other, gap)


def last_kernel(place, pieces, inverse, own, other, gap, out, coupling):
    r, k, _ = own.shape
    rows = (pieces.shape[1] - k) // 4
    solved = solve(pieces, 0, inverse, k, rows)
    turned = solved.T
    swapped = jnp.concatenate([turned[:, k:], turned[:, :k]], axis=1)
    coupling[...] = jnp.where(place[0] == 0, turned, swapped)
    high, low = split(solved)
    high, low = high.astype(BF), low.astype(BF)
    for i in range(r):
        both = jnp.concatenate([own[i], other[i]], axis=0)
        mixed = dot(high, both, TN) + dot(low, both, TN)
        value = (mixed - fock_rows(pieces, 0, i, k, rows)) / gap[i : i + 1, :]
        out[:, i, :] = value


def last_update(place, pieces, inverse, own, other, gap):
    r, k, n = own.shape
    vectors, coupling = pl.pallas_call(
        last_kernel,
        out_shape=(array((k, r, n), F32), array((k, 2 * k), F32)),
        in_specs=[SMEM] + [VMEM] * 5,
        out_specs=(VMEM, VMEM),
        compiler_params=PARAMS,
    )(place, pieces, inverse, own, other, gap)
    return vectors, coupling.T


def ring(step):
    pairs = []
    for h in range(4):
        for c in range(2):
            way = step if c == 1 else -step
            pairs.append((2 * h + c, 2 * ((h + way) % 4) + c))
    return pairs


AHEAD = ring(1)
BACK = ring(-1)
SIBLING = [(i, i ^ 1) for i in range(8)]
OTHER = [(0, 1), (1, 0)]


def per_device(factors, trial_vectors, energy_gap):
    place = jnp.stack([lax.axis_index(a) for a in ("gx", "gy", "gz")])
    own = jnp.transpose(trial_vectors, (1, 0, 2)).astype(BF)
    other = lax.ppermute(own, "gx", OTHER)
    b = jnp.transpose(factors, (1, 0, 2))

    def add(*terms):
        return sum(t.astype(F32) for t in terms).astype(BF)

    def fock_sums(own, other):
        (theirs,) = mix(place, own, b, True, BF, False)
        theirs = lax.ppermute(theirs, "gz", SIBLING)
        mine = mix(place, own, b, False, F32, True)
        gram = gram_parts(own, other, energy_gap)
        far = lax.ppermute(add(mine[0], theirs[0]), "gz", AHEAD)
        near = lax.ppermute(add(mine[2], theirs[2]), "gz", BACK)
        far = lax.ppermute(add(mine[1], theirs[1], far), "gz", AHEAD)
        first = add(mine[3], theirs[3], near, far)
        second = lax.ppermute(first, "gz", AHEAD)
        third = lax.ppermute(first, "gz", BACK)
        fourth = lax.ppermute(second, "gz", AHEAD)
        blocks = [first, second, third, fourth]
        blocks += [lax.ppermute(a, "gz", SIBLING) for a in blocks]
        fock, sums = fock_parts(place, blocks, b, own, other, gram)
        arrived = lax.all_to_all(fock.reshape(16, -1, fock.shape[1]), "gy", 0, 0, tiled=True)
        sums = sums + lax.ppermute(sums, "gz", SIBLING)
        sums = [sums] + [
            lax.ppermute(sums, "gz", [(i, i ^ flip) for i in range(8)]) for flip in (2, 4, 6)
        ]
        return arrived, sums

    for iteration in range(ITERS):
        last = iteration == ITERS - 1
        arrived, sums = fock_sums(own, other)
        pieces, totals = owner_sums(arrived, sums, 16 if last else 32)
        axes = "gy" if last else ("gx", "gy")
        pieces = lax.all_to_all(pieces, axes, 0, 0, tiled=True)
        inverse = inverse_of(totals)
        if last:
            return last_update(place, pieces, inverse, own, other, energy_gap)
        own, other = step_update(place, pieces, inverse, own, other, energy_gap)


def solution(mesh):
    placed = (P("gy", None, "gz"), P("gx", None, "gz"), P(None, "gz"))
    return jax.shard_map(
        per_device,
        mesh=mesh,
        in_specs=placed,
        out_specs=(P("gx", None, "gz"), P(None, "gx")),
        check_vma=False,
    )
```

```python
import jax
import jax.numpy as jnp
from jax import lax
from jax.experimental import pallas as pl
from jax.experimental.pallas import tpu as pltpu
from jax.sharding import PartitionSpec as P

ITERS = 2
BF = jnp.bfloat16
F32 = jnp.float32
HIGHEST = lax.Precision.HIGHEST


NT = (((1,), (1,)), ((), ()))
NN = (((1,), (0,)), ((), ()))
TN = (((0,), (0,)), ((), ()))


def dot(a, b, dims, precision=None):
    return lax.dot_general(a, b, dims, precision=precision, preferred_element_type=F32)


SMEM = pl.BlockSpec(memory_space=pltpu.SMEM)
VMEM = pl.BlockSpec(memory_space=pltpu.VMEM)
HBM = pl.BlockSpec(memory_space=pltpu.MemorySpace.HBM)
PARAMS = pltpu.CompilerParams(vmem_limit_bytes=24 << 20)


def array(shape, dtype):
    return jax.ShapeDtypeStruct(shape, dtype)


def split(value):
    high = value.astype(BF).astype(F32)
    return high, value - high


def lanes(value, parts):
    rows = value.shape[0] // parts
    return jnp.concatenate([value[i * rows : (i + 1) * rows] for i in range(parts)], axis=1)


def unlanes(value, parts):
    width = value.shape[1] // parts
    return jnp.concatenate([value[:, i * width : (i + 1) * width] for i in range(parts)], axis=0)


def rows_of(steps, place, sibling):
    chip = place >> 1
    core = (1 - (place & 1)) if sibling else (place & 1)
    way = 2 * core - 1
    return [2 * ((chip + s * way) & 3) + core for s in steps]


def fetch(source, order, buffer, arrivals):
    copies = [
        pltpu.make_async_copy(source.at[row], buffer.at[j], arrivals.at[j])
        for j, row in enumerate(order)
    ]
    for copy in copies:
        copy.start()
    return copies


def buffers(b):
    return [pltpu.VMEM(b.shape, b.dtype), pltpu.SemaphoreType.DMA((b.shape[0],))]


def mix_kernel(place, x, source, *refs, steps):
    *outs, b, arrivals = refs
    copies = fetch(source, range(source.shape[0]), b, arrivals)
    rows = x.shape[1]
    count = len(steps)
    order = rows_of(steps, place[2], True) + rows_of(steps, place[2], False)
    chosen = jnp.concatenate([x[j] for j in order], axis=0)
    for r in range(b.shape[0]):
        copies[r].wait()
        part = dot(chosen, b[r], NT)
        for j in range(count):
            theirs = part[j * rows : (j + 1) * rows]
            outs[0][j, r * rows : (r + 1) * rows, :] = theirs.astype(BF)
            mine = part[(count + j) * rows : (count + j + 1) * rows]
            outs[1 + j][r * rows : (r + 1) * rows, :] = mine


def mix(place, x, b, steps):
    r, k, _ = x.shape
    shape = (r * k, b.shape[1])
    outs = [array((len(steps), *shape), BF)] + [array(shape, F32)] * len(steps)
    return pl.pallas_call(
        lambda *refs: mix_kernel(*refs, steps=steps),
        out_shape=outs,
        in_specs=[SMEM, VMEM, HBM],
        out_specs=[VMEM] * len(outs),
        scratch_shapes=buffers(b),
        compiler_params=PARAMS,
    )(place, x, b)


def sums_kernel(place, own, other, gap, fock, message):
    r, k, _ = own.shape
    gram = jnp.zeros((2 * k, 2 * k), F32)
    scaled = jnp.zeros((2 * k, k), F32)
    projected = jnp.zeros((2 * k, k), F32)
    for i in range(r):
        both = jnp.concatenate([own[i], other[i]], axis=0)
        gram += dot(both, both, NT)
        high, low = split(own[i].astype(F32) * gap[i : i + 1, :])
        scaled += dot(both, high.astype(BF), NT) + dot(both, low.astype(BF), NT)
        projected += dot(both, fock[i * k : (i + 1) * k, :], NT)
    once = jnp.where(place[1] == 0, 1.0, 0.0)
    projected += once * scaled
    message[...] = jnp.concatenate([lanes(gram, 2), lanes(projected, 4)], axis=0)


def local_sums(place, own, other, gap, fock):
    k = own.shape[1]
    return pl.pallas_call(
        sums_kernel,
        out_shape=array((3 * k // 2, 4 * k), F32),
        in_specs=[SMEM] + [VMEM] * 4,
        out_specs=VMEM,
        compiler_params=PARAMS,
    )(place, own, other, gap, fock)


def fock_kernel(place, *refs):
    blocks = refs[:8]
    source, out, coulomb, b, arrivals = refs[8:]
    r, k, _ = coulomb.shape
    rows = r * k
    got = (0, -1, 1, 2)
    order = rows_of(got, place[2], False) + rows_of(got, place[2], True)
    copies = fetch(source, order, b, arrivals)
    fitted = jnp.zeros((k, b.shape[1]), F32)
    for j in range(8):
        start = pl.multiple_of(order[j] * k, k)
        fitted += blocks[j][pl.ds(start, k), :].astype(F32)
    fitted = fitted.astype(BF)
    total = jnp.zeros((rows, b.shape[2]), F32)
    for j in range(8):
        copies[j].wait()
        both = dot(jnp.concatenate([blocks[j][...], fitted], axis=0), b[j], NN)
        total += both[:rows]
        coulomb[order[j]] = both[rows:]
    for i in range(r):
        part = 2.0 * coulomb[i] - total[i * k : (i + 1) * k]
        out[i * k : (i + 1) * k, :] = part.astype(BF)


def fock_parts(place, blocks, b):
    r, _, n = b.shape
    rows = blocks[0].shape[0]
    return pl.pallas_call(
        fock_kernel,
        out_shape=array((rows, n), BF),
        in_specs=[SMEM] + [VMEM] * 8 + [HBM],
        out_specs=VMEM,
        scratch_shapes=[pltpu.VMEM((r, rows // r, n), F32)] + buffers(b),
        compiler_params=PARAMS,
    )(place, *blocks, b)


def owner_kernel(arrived, s0, s1, s2, s3, out, totals):
    total = (s0[...] + s1[...]) + (s2[...] + s3[...])
    size = totals.shape[0]
    totals[...] = total[:size]
    high, low = split(total[size:])
    tail = jnp.concatenate([high, low], axis=0).astype(BF)
    fock = arrived[0].astype(F32)
    for j in range(1, arrived.shape[0]):
        fock += arrived[j].astype(F32)
    fock = fock.astype(BF)
    rows = fock.shape[0]
    for p in range(out.shape[0]):
        for i in range(4):
            out[p, i * rows : (i + 1) * rows, :] = fock[:, i * 128 : (i + 1) * 128]
        out[p, 4 * rows :, :] = tail


def owner_sums(arrived, sums):
    copies, rows, _ = arrived.shape
    k = 2 * sums[0].shape[0] // 3
    return pl.pallas_call(
        owner_kernel,
        out_shape=(array((copies, 4 * rows + k, 128), BF), array((k, 128), F32)),
        in_specs=[VMEM] * 5,
        out_specs=(VMEM, VMEM),
        compiler_params=PARAMS,
    )(arrived, *sums)


def inverse_kernel(totals, out):
    size = 2 * totals.shape[0]
    half = unlanes(totals[...], 2)
    rows = lax.broadcasted_iota(jnp.int32, (size, 2 * size), 0)
    columns = lax.broadcasted_iota(jnp.int32, (size, 2 * size), 1)
    identity = (columns == rows + size).astype(F32)
    work = jnp.concatenate([half, identity[:, size:]], axis=1)
    for j in range(0, size, 2):
        first, second = work[j : j + 1], work[j + 1 : j + 2]
        aa, ab, bb = first[:, j : j + 1], first[:, j + 1 : j + 2], second[:, j + 1 : j + 2]
        scale = 1.0 / (aa * bb - ab * ab)
        top = (bb * scale) * first - (ab * scale) * second
        bottom = (aa * scale) * second - (ab * scale) * first
        rest = work - work[:, j : j + 1] * top - work[:, j + 1 : j + 2] * bottom
        work = jnp.where(rows == j, top, jnp.where(rows == j + 1, bottom, rest))
    out[...] = work[:, size:]


def inverse_of(totals):
    size = 2 * totals.shape[0]
    return pl.pallas_call(
        inverse_kernel,
        out_shape=array((size, size), F32),
        in_specs=[VMEM],
        out_specs=VMEM,
        compiler_params=PARAMS,
    )(totals)


def solve(pieces, inverse, k, rows):
    tail = jnp.zeros((k, 4 * k), F32)
    for j in range(pieces.shape[0]):
        tail += pieces[j, 4 * rows :, :].astype(F32)
    projected = unlanes(tail[: k // 2] + tail[k // 2 :], 4)
    return dot(inverse[...], projected, NN, HIGHEST)


def fock_rows(pieces, i, k, rows):
    per_row = k // rows
    parts = [lanes(pieces[i * per_row + h, : 4 * rows, :], 4) for h in range(per_row)]
    return jnp.concatenate(parts, axis=0).astype(F32)


def step_kernel(pieces, inverse, own, other, gap, out):
    r, k, _ = own.shape
    rows = (pieces.shape[1] - k) // 4
    high, low = split(solve(pieces, inverse, k, rows))
    high, low = high.astype(BF), low.astype(BF)
    for i in range(r):
        both = jnp.concatenate([own[i], other[i]], axis=0)
        mixed = dot(high, both, TN) + dot(low, both, TN)
        value = (mixed - fock_rows(pieces, i, k, rows)) / gap[i : i + 1, :]
        out[i] = value.astype(BF)


def step_update(pieces, inverse, own, other, gap):
    return pl.pallas_call(
        step_kernel,
        out_shape=array(own.shape, BF),
        in_specs=[VMEM] * 5,
        out_specs=VMEM,
        compiler_params=PARAMS,
    )(pieces, inverse, own, other, gap)


def last_kernel(place, pieces, inverse, own, other, gap, out, coupling):
    r, k, _ = own.shape
    rows = (pieces.shape[1] - k) // 4
    solved = solve(pieces, inverse, k, rows)
    turned = solved.T
    swapped = jnp.concatenate([turned[:, k:], turned[:, :k]], axis=1)
    coupling[...] = jnp.where(place[0] == 0, turned, swapped)
    high, low = split(solved)
    high, low = high.astype(BF), low.astype(BF)
    for i in range(r):
        both = jnp.concatenate([own[i], other[i]], axis=0)
        mixed = dot(high, both, TN) + dot(low, both, TN)
        value = (mixed - fock_rows(pieces, i, k, rows)) / gap[i : i + 1, :]
        out[:, i, :] = value


def last_update(place, pieces, inverse, own, other, gap):
    r, k, n = own.shape
    vectors, coupling = pl.pallas_call(
        last_kernel,
        out_shape=(array((k, r, n), F32), array((k, 2 * k), F32)),
        in_specs=[SMEM] + [VMEM] * 5,
        out_specs=(VMEM, VMEM),
        compiler_params=PARAMS,
    )(place, pieces, inverse, own, other, gap)
    return vectors, coupling.T


def ring(step):
    pairs = []
    for h in range(4):
        for c in range(2):
            way = step if c == 1 else -step
            pairs.append((2 * h + c, 2 * ((h + way) % 4) + c))
    return pairs


AHEAD = ring(1)
BACK = ring(-1)
SIBLING = [(i, i ^ 1) for i in range(8)]
OTHER = [(0, 1), (1, 0)]


def per_device(factors, trial_vectors, energy_gap):
    place = jnp.stack([lax.axis_index(a) for a in ("gx", "gy", "gz")])
    own = jnp.transpose(trial_vectors, (1, 0, 2)).astype(BF)
    b = pltpu.with_memory_space_constraint(jnp.transpose(factors, (1, 0, 2)), pltpu.HBM)

    def add(*terms):
        return sum(t.astype(F32) for t in terms).astype(BF)

    for iteration in range(ITERS):
        last = iteration == ITERS - 1
        theirs_far, mine_far = mix(place, own, b, (2,))
        theirs, *mine = mix(place, own, b, (-1, 1, 0))
        theirs_far = lax.ppermute(theirs_far, "gz", SIBLING)
        far = lax.ppermute(add(mine_far, theirs_far[0]), "gz", AHEAD)
        theirs = lax.ppermute(theirs, "gz", SIBLING)
        near = lax.ppermute(add(mine[0], theirs[0]), "gz", BACK)
        far = lax.ppermute(add(mine[1], theirs[1], far), "gz", AHEAD)
        first = add(mine[2], theirs[2], near, far)
        second = lax.ppermute(first, "gz", AHEAD)
        paired = lax.ppermute(first, "gz", SIBLING)
        third = lax.ppermute(first, "gz", BACK)
        fourth = lax.ppermute(second, "gz", AHEAD)
        other = lax.ppermute(own, "gx", OTHER)
        blocks = [first, second, third, fourth, paired]
        blocks += [lax.ppermute(a, "gz", SIBLING) for a in blocks[1:4]]
        fock = fock_parts(place, blocks, b)
        sums = local_sums(place, own, other, energy_gap, fock)
        arrived = lax.all_to_all(
            fock.reshape(16, -1, fock.shape[1]), "gy", 0, 0, tiled=True
        )
        sums = sums + lax.ppermute(sums, "gz", SIBLING)
        sums = [sums] + [
            lax.ppermute(sums, "gz", [(i, i ^ flip) for i in range(8)])
            for flip in (2, 4, 6)
        ]
        pieces, totals = owner_sums(arrived, sums)
        pieces = lax.all_to_all(pieces, "gy", 0, 0, tiled=True)
        inverse = inverse_of(totals)
        if last:
            return last_update(place, pieces, inverse, own, other, energy_gap)
        own = step_update(pieces, inverse, own, other, energy_gap)


def solution(mesh):
    placed = (P("gy", None, "gz"), P("gx", None, "gz"), P(None, "gz"))
    return jax.shard_map(
        per_device,
        mesh=mesh,
        in_specs=placed,
        out_specs=(P("gx", None, "gz"), P(None, "gx")),
        check_vma=False,
    )
```

```python
import jax
import jax.numpy as jnp
from jax import lax
from jax.experimental import pallas as pl
from jax.experimental.pallas import tpu as pltpu
from jax.sharding import PartitionSpec as P

ITERS = 2
BF = jnp.bfloat16
F32 = jnp.float32
HIGHEST = lax.Precision.HIGHEST


NT = (((1,), (1,)), ((), ()))
NN = (((1,), (0,)), ((), ()))
TN = (((0,), (0,)), ((), ()))


def dot(a, b, dims, precision=None):
    return lax.dot_general(a, b, dims, precision=precision, preferred_element_type=F32)


SMEM = pl.BlockSpec(memory_space=pltpu.SMEM)
VMEM = pl.BlockSpec(memory_space=pltpu.VMEM)
HBM = pl.BlockSpec(memory_space=pltpu.MemorySpace.HBM)
PARAMS = pltpu.CompilerParams(vmem_limit_bytes=24 << 20)


def array(shape, dtype):
    return jax.ShapeDtypeStruct(shape, dtype)


def split(value):
    high = value.astype(BF).astype(F32)
    return high, value - high


def lanes(value, parts):
    rows = value.shape[0] // parts
    return jnp.concatenate([value[i * rows : (i + 1) * rows] for i in range(parts)], axis=1)


def unlanes(value, parts):
    width = value.shape[1] // parts
    return jnp.concatenate([value[:, i * width : (i + 1) * width] for i in range(parts)], axis=0)


def rows_of(steps, place, sibling):
    chip = place >> 1
    core = (1 - (place & 1)) if sibling else (place & 1)
    way = 2 * core - 1
    return [2 * ((chip + s * way) & 3) + core for s in steps]


def fetch(source, order, buffer, arrivals):
    copies = [
        pltpu.make_async_copy(source.at[row], buffer.at[j], arrivals.at[j])
        for j, row in enumerate(order)
    ]
    for copy in copies:
        copy.start()
    return copies


def buffers(b):
    return [pltpu.VMEM(b.shape, b.dtype), pltpu.SemaphoreType.DMA((b.shape[0],))]


def mix_kernel(place, x, held, source, *refs, steps):
    *outs, streamed, arrivals = refs
    copies = fetch(source, range(source.shape[0]), streamed, arrivals)
    rows = x.shape[1]
    count = len(steps)
    order = rows_of(steps, place[2], True) + rows_of(steps, place[2], False)
    chosen = jnp.concatenate([x[j] for j in order], axis=0)
    middle = held.shape[1]

    def put(r, columns, part):
        for j in range(count):
            theirs = part[j * rows : (j + 1) * rows]
            outs[0][j, r * rows : (r + 1) * rows, columns] = theirs.astype(BF)
            mine = part[(count + j) * rows : (count + j + 1) * rows]
            outs[1 + j][r * rows : (r + 1) * rows, columns] = mine

    for r in range(held.shape[0]):
        put(r, slice(0, middle), dot(chosen, held[r], NT))
    for r in range(held.shape[0]):
        copies[r].wait()
        put(r, slice(middle, outs[0].shape[2]), dot(chosen, streamed[r], NT))


def mix(place, x, b, steps):
    r, k, _ = x.shape
    shape = (r * k, b[0].shape[1] + b[1].shape[1])
    outs = [array((len(steps), *shape), BF)] + [array(shape, F32)] * len(steps)
    return pl.pallas_call(
        lambda *refs: mix_kernel(*refs, steps=steps),
        out_shape=outs,
        in_specs=[SMEM, VMEM, VMEM, HBM],
        out_specs=[VMEM] * len(outs),
        scratch_shapes=buffers(b[1]),
        compiler_params=PARAMS,
    )(place, x, *b)


def add_kernel(mine, theirs, *refs):
    *others, out = refs
    total = mine[...] + theirs[0].astype(F32)
    for other in others:
        total += other[...].astype(F32)
    out[...] = total.astype(BF)


def add(mine, theirs, index, *others):
    whole = pl.BlockSpec(mine.shape, lambda i: (0, 0))
    return pl.pallas_call(
        add_kernel,
        grid=(1,),
        out_shape=array(mine.shape, BF),
        in_specs=[whole, pl.BlockSpec((1, *mine.shape), lambda i: (index, 0, 0))]
        + [whole] * len(others),
        out_specs=whole,
        compiler_params=PARAMS,
    )(mine, theirs, *others)


def sums_kernel(place, own, other, gap, fock, message):
    r, k, _ = own.shape
    gram = jnp.zeros((2 * k, 2 * k), F32)
    scaled = jnp.zeros((2 * k, k), F32)
    projected = jnp.zeros((2 * k, k), F32)
    for i in range(r):
        both = jnp.concatenate([own[i], other[i]], axis=0)
        gram += dot(both, both, NT)
        high, low = split(own[i].astype(F32) * gap[i : i + 1, :])
        scaled += dot(both, high.astype(BF), NT) + dot(both, low.astype(BF), NT)
        projected += dot(both, fock[i * k : (i + 1) * k, :], NT)
    once = jnp.where(place[1] == 0, 1.0, 0.0)
    projected += once * scaled
    message[...] = jnp.concatenate([lanes(gram, 2), lanes(projected, 4)], axis=0)


def local_sums(place, own, other, gap, fock):
    k = own.shape[1]
    return pl.pallas_call(
        sums_kernel,
        out_shape=array((3 * k // 2, 4 * k), F32),
        in_specs=[SMEM] + [VMEM] * 4,
        out_specs=VMEM,
        compiler_params=PARAMS,
    )(place, own, other, gap, fock)


def fock_kernel(place, *refs):
    blocks = refs[:8]
    held, source, out, coulomb, streamed, arrivals = refs[8:]
    r, k, _ = coulomb.shape
    rows = r * k
    got = (0, -1, 1, 2)
    order = rows_of(got, place[2], False) + rows_of(got, place[2], True)
    copies = fetch(source, order, streamed, arrivals)
    fitted = jnp.zeros((k, blocks[0].shape[1]), F32)
    for j in range(8):
        start = pl.multiple_of(order[j] * k, k)
        fitted += blocks[j][pl.ds(start, k), :].astype(F32)
    fitted = fitted.astype(BF)
    middle = held.shape[1]
    total = jnp.zeros((rows, held.shape[2]), F32)
    for j in range(8):
        left = jnp.concatenate([blocks[j][:, :middle], fitted[:, :middle]], axis=0)
        both = dot(left, held[order[j]], NN)
        total += both[:rows]
        coulomb[order[j]] = both[rows:]
    for j in range(8):
        copies[j].wait()
        left = jnp.concatenate([blocks[j][:, middle:], fitted[:, middle:]], axis=0)
        both = dot(left, streamed[j], NN)
        total += both[:rows]
        coulomb[order[j]] += both[rows:]
    for i in range(r):
        part = 2.0 * coulomb[i] - total[i * k : (i + 1) * k]
        out[i * k : (i + 1) * k, :] = part.astype(BF)


def fock_parts(place, blocks, b):
    r, _, n = b[0].shape
    rows = blocks[0].shape[0]
    return pl.pallas_call(
        fock_kernel,
        out_shape=array((rows, n), BF),
        in_specs=[SMEM] + [VMEM] * 9 + [HBM],
        out_specs=VMEM,
        scratch_shapes=[pltpu.VMEM((r, rows // r, n), F32)] + buffers(b[1]),
        compiler_params=PARAMS,
    )(place, *blocks, *b)


def owner_kernel(arrived, s0, s1, s2, s3, out, totals):
    total = (s0[...] + s1[...]) + (s2[...] + s3[...])
    size = totals.shape[0]
    totals[...] = total[:size]
    high, low = split(total[size:])
    tail = jnp.concatenate([high, low], axis=0).astype(BF)
    fock = arrived[0].astype(F32)
    for j in range(1, arrived.shape[0]):
        fock += arrived[j].astype(F32)
    fock = fock.astype(BF)
    rows = fock.shape[0]
    for p in range(out.shape[0]):
        for i in range(4):
            out[p, i * rows : (i + 1) * rows, :] = fock[:, i * 128 : (i + 1) * 128]
        out[p, 4 * rows :, :] = tail


def owner_sums(arrived, sums):
    copies, rows, _ = arrived.shape
    k = 2 * sums[0].shape[0] // 3
    return pl.pallas_call(
        owner_kernel,
        out_shape=(array((copies, 4 * rows + k, 128), BF), array((k, 128), F32)),
        in_specs=[VMEM] * 5,
        out_specs=(VMEM, VMEM),
        compiler_params=PARAMS,
    )(arrived, *sums)


def inverse_kernel(totals, out):
    size = 2 * totals.shape[0]
    half = unlanes(totals[...], 2)
    rows = lax.broadcasted_iota(jnp.int32, (size, 2 * size), 0)
    columns = lax.broadcasted_iota(jnp.int32, (size, 2 * size), 1)
    identity = (columns == rows + size).astype(F32)
    work = jnp.concatenate([half, identity[:, size:]], axis=1)
    for j in range(0, size, 2):
        first, second = work[j : j + 1], work[j + 1 : j + 2]
        aa, ab, bb = first[:, j : j + 1], first[:, j + 1 : j + 2], second[:, j + 1 : j + 2]
        scale = 1.0 / (aa * bb - ab * ab)
        top = (bb * scale) * first - (ab * scale) * second
        bottom = (aa * scale) * second - (ab * scale) * first
        rest = work - work[:, j : j + 1] * top - work[:, j + 1 : j + 2] * bottom
        work = jnp.where(rows == j, top, jnp.where(rows == j + 1, bottom, rest))
    out[...] = work[:, size:]


def inverse_of(totals):
    size = 2 * totals.shape[0]
    return pl.pallas_call(
        inverse_kernel,
        out_shape=array((size, size), F32),
        in_specs=[VMEM],
        out_specs=VMEM,
        compiler_params=PARAMS,
    )(totals)


def solve(pieces, inverse, k, rows):
    tail = jnp.zeros((k, 4 * k), F32)
    for j in range(pieces.shape[0]):
        tail += pieces[j, 4 * rows :, :].astype(F32)
    projected = unlanes(tail[: k // 2] + tail[k // 2 :], 4)
    return dot(inverse[...], projected, NN, HIGHEST)


def fock_rows(pieces, i, k, rows):
    per_row = k // rows
    parts = [lanes(pieces[i * per_row + h, : 4 * rows, :], 4) for h in range(per_row)]
    return jnp.concatenate(parts, axis=0).astype(F32)


def step_kernel(pieces, inverse, own, other, gap, out):
    r, k, _ = own.shape
    rows = (pieces.shape[1] - k) // 4
    high, low = split(solve(pieces, inverse, k, rows))
    high, low = high.astype(BF), low.astype(BF)
    for i in range(r):
        both = jnp.concatenate([own[i], other[i]], axis=0)
        mixed = dot(high, both, TN) + dot(low, both, TN)
        value = (mixed - fock_rows(pieces, i, k, rows)) / gap[i : i + 1, :]
        out[i] = value.astype(BF)


def step_update(pieces, inverse, own, other, gap):
    return pl.pallas_call(
        step_kernel,
        out_shape=array(own.shape, BF),
        in_specs=[VMEM] * 5,
        out_specs=VMEM,
        compiler_params=PARAMS,
    )(pieces, inverse, own, other, gap)


def last_kernel(place, pieces, inverse, own, other, gap, out, coupling):
    r, k, _ = own.shape
    rows = (pieces.shape[1] - k) // 4
    solved = solve(pieces, inverse, k, rows)
    turned = solved.T
    swapped = jnp.concatenate([turned[:, k:], turned[:, :k]], axis=1)
    coupling[...] = jnp.where(place[0] == 0, turned, swapped)
    high, low = split(solved)
    high, low = high.astype(BF), low.astype(BF)
    for i in range(r):
        both = jnp.concatenate([own[i], other[i]], axis=0)
        mixed = dot(high, both, TN) + dot(low, both, TN)
        value = (mixed - fock_rows(pieces, i, k, rows)) / gap[i : i + 1, :]
        out[:, i, :] = value


def last_update(place, pieces, inverse, own, other, gap):
    r, k, n = own.shape
    vectors, coupling = pl.pallas_call(
        last_kernel,
        out_shape=(array((k, r, n), F32), array((k, 2 * k), F32)),
        in_specs=[SMEM] + [VMEM] * 5,
        out_specs=(VMEM, VMEM),
        compiler_params=PARAMS,
    )(place, pieces, inverse, own, other, gap)
    return vectors, coupling.T


def ring(step):
    pairs = []
    for h in range(4):
        for c in range(2):
            way = step if c == 1 else -step
            pairs.append((2 * h + c, 2 * ((h + way) % 4) + c))
    return pairs


AHEAD = ring(1)
BACK = ring(-1)
SIBLING = [(i, i ^ 1) for i in range(8)]
OTHER = [(0, 1), (1, 0)]


def per_device(factors, trial_vectors, energy_gap):
    place = jnp.stack([lax.axis_index(a) for a in ("gx", "gy", "gz")])
    own = jnp.transpose(trial_vectors, (1, 0, 2)).astype(BF)
    middle = 2 * factors.shape[0] // 3
    held = jnp.transpose(factors[:middle], (1, 0, 2))
    streamed = jnp.transpose(factors[middle:], (1, 0, 2))
    b = held, pltpu.with_memory_space_constraint(streamed, pltpu.HBM)

    for iteration in range(ITERS):
        last = iteration == ITERS - 1
        theirs_far, mine_far = mix(place, own, b, (2,))
        theirs, *mine = mix(place, own, b, (-1, 1, 0))
        theirs_far = lax.ppermute(theirs_far, "gz", SIBLING)
        far = lax.ppermute(add(mine_far, theirs_far, 0), "gz", AHEAD)
        theirs = lax.ppermute(theirs, "gz", SIBLING)
        near = lax.ppermute(add(mine[0], theirs, 0), "gz", BACK)
        far = lax.ppermute(add(mine[1], theirs, 1, far), "gz", AHEAD)
        first = add(mine[2], theirs, 2, near, far)
        second = lax.ppermute(first, "gz", AHEAD)
        paired = lax.ppermute(first, "gz", SIBLING)
        third = lax.ppermute(first, "gz", BACK)
        fourth = lax.ppermute(second, "gz", AHEAD)
        other = lax.ppermute(own, "gx", OTHER)
        blocks = [first, second, third, fourth, paired]
        blocks += [lax.ppermute(a, "gz", SIBLING) for a in blocks[1:4]]
        fock = fock_parts(place, blocks, b)
        sums = local_sums(place, own, other, energy_gap, fock)
        arrived = lax.all_to_all(
            fock.reshape(16, -1, fock.shape[1]), "gy", 0, 0, tiled=True
        )
        sums = sums + lax.ppermute(sums, "gz", SIBLING)
        sums = [sums] + [
            lax.ppermute(sums, "gz", [(i, i ^ flip) for i in range(8)])
            for flip in (2, 4, 6)
        ]
        pieces, totals = owner_sums(arrived, sums)
        pieces = lax.all_to_all(pieces, "gy", 0, 0, tiled=True)
        inverse = inverse_of(totals)
        if last:
            return last_update(place, pieces, inverse, own, other, energy_gap)
        own = step_update(pieces, inverse, own, other, energy_gap)


def solution(mesh):
    placed = (P("gy", None, "gz"), P("gx", None, "gz"), P(None, "gz"))
    return jax.shard_map(
        per_device,
        mesh=mesh,
        in_specs=placed,
        out_specs=(P("gx", None, "gz"), P(None, "gx")),
        check_vma=False,
    )
```

```python
import jax
import jax.numpy as jnp
from jax import lax
from jax.experimental import pallas as pl
from jax.experimental.pallas import tpu as pltpu
from jax.sharding import PartitionSpec as P

ITERS = 2
BF = jnp.bfloat16
F32 = jnp.float32
HIGHEST = lax.Precision.HIGHEST


NT = (((1,), (1,)), ((), ()))
NN = (((1,), (0,)), ((), ()))
TN = (((0,), (0,)), ((), ()))


def dot(a, b, dims, precision=None):
    return lax.dot_general(a, b, dims, precision=precision, preferred_element_type=F32)


SMEM = pl.BlockSpec(memory_space=pltpu.SMEM)
VMEM = pl.BlockSpec(memory_space=pltpu.VMEM)
PARAMS = pltpu.CompilerParams(vmem_limit_bytes=24 << 20)


def array(shape, dtype):
    return jax.ShapeDtypeStruct(shape, dtype)


def split(value):
    high = value.astype(BF).astype(F32)
    return high, value - high


def lanes(value, parts):
    rows = value.shape[0] // parts
    return jnp.concatenate([value[i * rows : (i + 1) * rows] for i in range(parts)], axis=1)


def unlanes(value, parts):
    width = value.shape[1] // parts
    return jnp.concatenate([value[:, i * width : (i + 1) * width] for i in range(parts)], axis=0)


def rows_of(steps, place, sibling):
    chip = place >> 1
    core = (1 - (place & 1)) if sibling else (place & 1)
    way = 2 * core - 1
    return [2 * ((chip + s * way) & 3) + core for s in steps]


def mix_kernel(place, x, b, *outs, steps):
    rows = x.shape[1]
    count = len(steps)
    order = rows_of(steps, place[2], True) + rows_of(steps, place[2], False)
    chosen = jnp.concatenate([x[j] for j in order], axis=0)
    for r in range(b.shape[0]):
        part = dot(chosen, b[r], NT)
        for j in range(count):
            theirs = part[j * rows : (j + 1) * rows]
            outs[0][j, r * rows : (r + 1) * rows, :] = theirs.astype(BF)
            mine = part[(count + j) * rows : (count + j + 1) * rows]
            outs[1 + j][r * rows : (r + 1) * rows, :] = mine


def mix(place, x, b, steps):
    r, k, _ = x.shape
    shape = (r * k, b.shape[1])
    outs = [array((len(steps), *shape), BF)] + [array(shape, F32)] * len(steps)
    return pl.pallas_call(
        lambda *refs: mix_kernel(*refs, steps=steps),
        out_shape=outs,
        in_specs=[SMEM, VMEM, VMEM],
        out_specs=[VMEM] * len(outs),
        compiler_params=PARAMS,
    )(place, x, b)


def add_kernel(mine, theirs, *refs):
    *others, out = refs
    total = mine[...] + theirs[0].astype(F32)
    for other in others:
        total += other[...].astype(F32)
    out[...] = total.astype(BF)


def add(mine, theirs, index, *others):
    whole = pl.BlockSpec(mine.shape, lambda i: (0, 0))
    return pl.pallas_call(
        add_kernel,
        grid=(1,),
        out_shape=array(mine.shape, BF),
        in_specs=[whole, pl.BlockSpec((1, *mine.shape), lambda i: (index, 0, 0))]
        + [whole] * len(others),
        out_specs=whole,
        compiler_params=PARAMS,
    )(mine, theirs, *others)


def sums_kernel(place, own, other, gap, fock, message):
    r, k, _ = own.shape
    gram = jnp.zeros((2 * k, 2 * k), F32)
    scaled = jnp.zeros((2 * k, k), F32)
    projected = jnp.zeros((2 * k, k), F32)
    for i in range(r):
        both = jnp.concatenate([own[i], other[i]], axis=0)
        gram += dot(both, both, NT)
        high, low = split(own[i].astype(F32) * gap[i : i + 1, :])
        scaled += dot(both, high.astype(BF), NT) + dot(both, low.astype(BF), NT)
        projected += dot(both, fock[i * k : (i + 1) * k, :], NT)
    once = jnp.where(place[1] == 0, 1.0, 0.0)
    projected += once * scaled
    message[...] = jnp.concatenate([lanes(gram, 2), lanes(projected, 4)], axis=0)


def local_sums(place, own, other, gap, fock):
    k = own.shape[1]
    return pl.pallas_call(
        sums_kernel,
        out_shape=array((3 * k // 2, 4 * k), F32),
        in_specs=[SMEM] + [VMEM] * 4,
        out_specs=VMEM,
        compiler_params=PARAMS,
    )(place, own, other, gap, fock)


def fock_kernel(place, *refs):
    blocks = refs[:8]
    b, out, coulomb = refs[8:]
    r, k, _ = coulomb.shape
    rows = r * k
    got = (0, -1, 1, 2)
    order = rows_of(got, place[2], False) + rows_of(got, place[2], True)
    fitted = jnp.zeros((k, blocks[0].shape[1]), F32)
    for j in range(8):
        start = pl.multiple_of(order[j] * k, k)
        fitted += blocks[j][pl.ds(start, k), :].astype(F32)
    fitted = fitted.astype(BF)
    total = jnp.zeros((rows, b.shape[2]), F32)
    for j in range(8):
        both = dot(jnp.concatenate([blocks[j][...], fitted], axis=0), b[order[j]], NN)
        total += both[:rows]
        coulomb[order[j]] = both[rows:]
    for i in range(r):
        part = 2.0 * coulomb[i] - total[i * k : (i + 1) * k]
        out[i * k : (i + 1) * k, :] = part.astype(BF)


def fock_parts(place, blocks, b):
    r, _, n = b.shape
    rows = blocks[0].shape[0]
    return pl.pallas_call(
        fock_kernel,
        out_shape=array((rows, n), BF),
        in_specs=[SMEM] + [VMEM] * 9,
        out_specs=VMEM,
        scratch_shapes=[pltpu.VMEM((r, rows // r, n), F32)],
        compiler_params=PARAMS,
    )(place, *blocks, b)


def owner_kernel(arrived, s0, s1, s2, s3, out, totals):
    total = (s0[...] + s1[...]) + (s2[...] + s3[...])
    size = totals.shape[0]
    totals[...] = total[:size]
    high, low = split(total[size:])
    tail = jnp.concatenate([high, low], axis=0).astype(BF)
    fock = arrived[0].astype(F32)
    for j in range(1, arrived.shape[0]):
        fock += arrived[j].astype(F32)
    fock = fock.astype(BF)
    rows = fock.shape[0]
    for p in range(out.shape[0]):
        for i in range(4):
            out[p, i * rows : (i + 1) * rows, :] = fock[:, i * 128 : (i + 1) * 128]
        out[p, 4 * rows :, :] = tail


def owner_sums(arrived, sums, keep):
    copies, rows, _ = arrived.shape
    k = 2 * sums[0].shape[0] // 3
    return pl.pallas_call(
        owner_kernel,
        out_shape=(array((copies, 4 * rows + k, 128), BF), keep((k, 128), F32)),
        in_specs=[VMEM] * 5,
        out_specs=(VMEM, VMEM),
        compiler_params=PARAMS,
    )(arrived, *sums)


def inverse_kernel(totals, out):
    size = 2 * totals.shape[0]
    half = unlanes(totals[...], 2)
    rows = lax.broadcasted_iota(jnp.int32, (size, 2 * size), 0)
    columns = lax.broadcasted_iota(jnp.int32, (size, 2 * size), 1)
    identity = (columns == rows + size).astype(F32)
    work = jnp.concatenate([half, identity[:, size:]], axis=1)
    for j in range(0, size, 2):
        first, second = work[j : j + 1], work[j + 1 : j + 2]
        aa, ab, bb = first[:, j : j + 1], first[:, j + 1 : j + 2], second[:, j + 1 : j + 2]
        scale = 1.0 / (aa * bb - ab * ab)
        top = (bb * scale) * first - (ab * scale) * second
        bottom = (aa * scale) * second - (ab * scale) * first
        rest = work - work[:, j : j + 1] * top - work[:, j + 1 : j + 2] * bottom
        work = jnp.where(rows == j, top, jnp.where(rows == j + 1, bottom, rest))
    out[...] = work[:, size:]


def inverse_of(totals, keep):
    size = 2 * totals.shape[0]
    return pl.pallas_call(
        inverse_kernel,
        out_shape=keep((size, size), F32),
        in_specs=[VMEM],
        out_specs=VMEM,
        compiler_params=PARAMS,
    )(totals)


def solve(pieces, inverse, k, rows):
    tail = jnp.zeros((k, 4 * k), F32)
    for j in range(pieces.shape[0]):
        tail += pieces[j, 4 * rows :, :].astype(F32)
    projected = unlanes(tail[: k // 2] + tail[k // 2 :], 4)
    return dot(inverse[...], projected, NN, HIGHEST)


def fock_rows(pieces, i, k, rows):
    per_row = k // rows
    parts = [lanes(pieces[i * per_row + h, : 4 * rows, :], 4) for h in range(per_row)]
    return jnp.concatenate(parts, axis=0).astype(F32)


def step_kernel(pieces, inverse, own, other, gap, out):
    r, k, _ = own.shape
    rows = (pieces.shape[1] - k) // 4
    high, low = split(solve(pieces, inverse, k, rows))
    high, low = high.astype(BF), low.astype(BF)
    for i in range(r):
        both = jnp.concatenate([own[i], other[i]], axis=0)
        mixed = dot(high, both, TN) + dot(low, both, TN)
        value = (mixed - fock_rows(pieces, i, k, rows)) / gap[i : i + 1, :]
        out[i] = value.astype(BF)


def step_update(pieces, inverse, own, other, gap):
    return pl.pallas_call(
        step_kernel,
        out_shape=array(own.shape, BF),
        in_specs=[VMEM] * 5,
        out_specs=VMEM,
        compiler_params=PARAMS,
    )(pieces, inverse, own, other, gap)


def last_kernel(place, pieces, inverse, own, other, gap, out, coupling):
    r, k, _ = own.shape
    rows = (pieces.shape[1] - k) // 4
    solved = solve(pieces, inverse, k, rows)
    turned = solved.T
    swapped = jnp.concatenate([turned[:, k:], turned[:, :k]], axis=1)
    coupling[...] = jnp.where(place[0] == 0, turned, swapped)
    high, low = split(solved)
    high, low = high.astype(BF), low.astype(BF)
    for i in range(r):
        both = jnp.concatenate([own[i], other[i]], axis=0)
        mixed = dot(high, both, TN) + dot(low, both, TN)
        value = (mixed - fock_rows(pieces, i, k, rows)) / gap[i : i + 1, :]
        out[:, i, :] = value


def last_update(place, pieces, inverse, own, other, gap):
    r, k, n = own.shape
    vectors, coupling = pl.pallas_call(
        last_kernel,
        out_shape=(array((k, r, n), F32), array((k, 2 * k), F32)),
        in_specs=[SMEM] + [VMEM] * 5,
        out_specs=(VMEM, VMEM),
        compiler_params=PARAMS,
    )(place, pieces, inverse, own, other, gap)
    return vectors, coupling.T


def ring(step):
    pairs = []
    for h in range(4):
        for c in range(2):
            way = step if c == 1 else -step
            pairs.append((2 * h + c, 2 * ((h + way) % 4) + c))
    return pairs


AHEAD = ring(1)
BACK = ring(-1)
SIBLING = [(i, i ^ 1) for i in range(8)]
OTHER = [(0, 1), (1, 0)]


def in_hbm(value):
    return pltpu.with_memory_space_constraint(value, pltpu.HBM)


def per_device(factors, trial_vectors, energy_gap):
    place = jnp.stack([lax.axis_index(a) for a in ("gx", "gy", "gz")])
    own = jnp.transpose(trial_vectors, (1, 0, 2)).astype(BF)
    b = jnp.transpose(factors, (1, 0, 2))

    for iteration in range(ITERS):
        last = iteration == ITERS - 1
        theirs_far, mine_far = mix(place, own, b, (2,))
        theirs, *mine = mix(place, own, b, (-1, 1, 0))
        theirs_far = lax.ppermute(theirs_far, "gz", SIBLING)
        far = lax.ppermute(add(mine_far, theirs_far, 0), "gz", AHEAD)
        theirs = lax.ppermute(theirs, "gz", SIBLING)
        near = lax.ppermute(add(mine[0], theirs, 0), "gz", BACK)
        far = lax.ppermute(add(mine[1], theirs, 1, far), "gz", AHEAD)
        first = add(mine[2], theirs, 2, near, far)
        second = lax.ppermute(first, "gz", AHEAD)
        paired = lax.ppermute(first, "gz", SIBLING)
        third = lax.ppermute(first, "gz", BACK)
        fourth = lax.ppermute(second, "gz", AHEAD)
        other = lax.ppermute(own, "gx", OTHER)
        blocks = [first, second, third, fourth, paired]
        blocks += [lax.ppermute(a, "gz", SIBLING) for a in blocks[1:4]]
        fock = fock_parts(place, blocks, b)
        sums = local_sums(place, own, other, energy_gap, fock)
        arrived = lax.all_to_all(
            fock.reshape(16, -1, fock.shape[1]), "gy", 0, 0, tiled=True
        )
        sums = sums + lax.ppermute(sums, "gz", SIBLING)
        sums = [sums] + [
            lax.ppermute(sums, "gz", [(i, i ^ flip) for i in range(8)])
            for flip in (2, 4, 6)
        ]
        own, other = in_hbm(own), in_hbm(other)
        keep = array if last else pltpu.HBM
        pieces, totals = owner_sums(arrived, sums, keep)
        pieces = lax.all_to_all(pieces, "gy", 0, 0, tiled=True)
        inverse = inverse_of(totals if last else in_hbm(totals), keep)
        if last:
            return last_update(place, pieces, inverse, own, other, energy_gap)
        own = step_update(in_hbm(pieces), in_hbm(inverse), own, other, energy_gap)


def solution(mesh):
    placed = (P("gy", None, "gz"), P("gx", None, "gz"), P(None, "gz"))
    return jax.shard_map(
        per_device,
        mesh=mesh,
        in_specs=placed,
        out_specs=(P("gx", None, "gz"), P(None, "gx")),
        check_vma=False,
    )
```

```python
import jax
import jax.numpy as jnp
from jax import lax
from jax.experimental import pallas as pl
from jax.experimental.pallas import tpu as pltpu
from jax.sharding import PartitionSpec as P

ITERS = 2
BF = jnp.bfloat16
F32 = jnp.float32
HIGHEST = lax.Precision.HIGHEST


NT = (((1,), (1,)), ((), ()))
NN = (((1,), (0,)), ((), ()))
TN = (((0,), (0,)), ((), ()))


def dot(a, b, dims, precision=None):
    return lax.dot_general(a, b, dims, precision=precision, preferred_element_type=F32)


SMEM = pl.BlockSpec(memory_space=pltpu.SMEM)
VMEM = pl.BlockSpec(memory_space=pltpu.VMEM)
PARAMS = pltpu.CompilerParams(vmem_limit_bytes=24 << 20)


def array(shape, dtype):
    return jax.ShapeDtypeStruct(shape, dtype)


def split(value):
    high = value.astype(BF).astype(F32)
    return high, value - high


def lanes(value, parts):
    rows = value.shape[0] // parts
    return jnp.concatenate([value[i * rows : (i + 1) * rows] for i in range(parts)], axis=1)


def unlanes(value, parts):
    width = value.shape[1] // parts
    return jnp.concatenate([value[:, i * width : (i + 1) * width] for i in range(parts)], axis=0)


def rows_of(steps, place, sibling):
    chip = place >> 1
    core = (1 - (place & 1)) if sibling else (place & 1)
    way = 2 * core - 1
    return [2 * ((chip + s * way) & 3) + core for s in steps]


def mix_kernel(place, x, b, *outs, steps):
    rows = x.shape[1]
    count = len(steps)
    order = rows_of(steps, place[2], True) + rows_of(steps, place[2], False)
    chosen = jnp.concatenate([x[j] for j in order], axis=0)
    for r in range(b.shape[0]):
        part = dot(chosen, b[r], NT)
        for j in range(count):
            theirs = part[j * rows : (j + 1) * rows]
            outs[0][j, r * rows : (r + 1) * rows, :] = theirs.astype(BF)
            mine = part[(count + j) * rows : (count + j + 1) * rows]
            outs[1 + j][r * rows : (r + 1) * rows, :] = mine


def mix(place, x, b, steps):
    r, k, _ = x.shape
    shape = (r * k, b.shape[1])
    outs = [array((len(steps), *shape), BF)] + [array(shape, F32)] * len(steps)
    return pl.pallas_call(
        lambda *refs: mix_kernel(*refs, steps=steps),
        out_shape=outs,
        in_specs=[SMEM, VMEM, VMEM],
        out_specs=[VMEM] * len(outs),
        compiler_params=PARAMS,
    )(place, x, b)


def add_kernel(mine, theirs, *refs):
    *others, out = refs
    total = mine[...] + theirs[0].astype(F32)
    for other in others:
        total += other[...].astype(F32)
    out[...] = total.astype(BF)


def add(mine, theirs, index, *others):
    whole = pl.BlockSpec(mine.shape, lambda i: (0, 0))
    return pl.pallas_call(
        add_kernel,
        grid=(1,),
        out_shape=array(mine.shape, BF),
        in_specs=[whole, pl.BlockSpec((1, *mine.shape), lambda i: (index, 0, 0))]
        + [whole] * len(others),
        out_specs=whole,
        compiler_params=PARAMS,
    )(mine, theirs, *others)


def gram_kernel(own, other, gap, out):
    r, k, _ = own.shape
    gram = jnp.zeros((2 * k, 2 * k), F32)
    scaled = jnp.zeros((2 * k, k), F32)
    for i in range(r):
        both = jnp.concatenate([own[i], other[i]], axis=0)
        gram += dot(both, both, NT)
        high, low = split(own[i].astype(F32) * gap[i : i + 1, :])
        scaled += dot(both, high.astype(BF), NT) + dot(both, low.astype(BF), NT)
    out[...] = jnp.concatenate([gram, scaled], axis=1)


def gram_parts(own, other, gap):
    k = own.shape[1]
    return pl.pallas_call(
        gram_kernel,
        out_shape=array((2 * k, 3 * k), F32),
        in_specs=[VMEM] * 3,
        out_specs=VMEM,
        compiler_params=PARAMS,
    )(own, other, gap)


def fock_kernel(place, *refs):
    blocks = refs[:8]
    b, own, other, gram, out, message, coulomb = refs[8:]
    r, k, _ = own.shape
    rows = r * k
    got = (0, -1, 1, 2)
    order = rows_of(got, place[2], False) + rows_of(got, place[2], True)
    fitted = jnp.zeros((k, blocks[0].shape[1]), F32)
    for j in range(8):
        start = pl.multiple_of(order[j] * k, k)
        fitted += blocks[j][pl.ds(start, k), :].astype(F32)
    fitted = fitted.astype(BF)
    total = jnp.zeros((rows, b.shape[2]), F32)
    for j in range(8):
        both = dot(jnp.concatenate([blocks[j][...], fitted], axis=0), b[order[j]], NN)
        total += both[:rows]
        coulomb[order[j]] = both[rows:]
    projected = jnp.zeros((2 * k, k), F32)
    for i in range(r):
        part = 2.0 * coulomb[i] - total[i * k : (i + 1) * k]
        part = part.astype(BF)
        out[i * k : (i + 1) * k, :] = part
        projected += dot(jnp.concatenate([own[i], other[i]], axis=0), part, NT)
    once = jnp.where(place[1] == 0, 1.0, 0.0)
    projected += once * gram[:, 2 * k :]
    message[...] = jnp.concatenate([lanes(gram[:, : 2 * k], 2), lanes(projected, 4)], axis=0)


def fock_parts(place, blocks, b, own, other, gram):
    r, k, n = own.shape
    return pl.pallas_call(
        fock_kernel,
        out_shape=(array((r * k, n), BF), array((3 * k // 2, 4 * k), F32)),
        in_specs=[SMEM] + [VMEM] * 12,
        out_specs=(VMEM, VMEM),
        scratch_shapes=[pltpu.VMEM((r, k, n), F32)],
        compiler_params=PARAMS,
    )(place, *blocks, b, own, other, gram)


def owner_kernel(arrived, s0, s1, s2, s3, out, totals):
    total = (s0[...] + s1[...]) + (s2[...] + s3[...])
    size = totals.shape[0]
    totals[...] = total[:size]
    high, low = split(total[size:])
    tail = jnp.concatenate([high, low], axis=0).astype(BF)
    fock = arrived[0].astype(F32)
    for j in range(1, arrived.shape[0]):
        fock += arrived[j].astype(F32)
    fock = fock.astype(BF)
    rows = fock.shape[0]
    for p in range(out.shape[0]):
        for i in range(4):
            out[p, i * rows : (i + 1) * rows, :] = fock[:, i * 128 : (i + 1) * 128]
        out[p, 4 * rows :, :] = tail


def owner_sums(arrived, sums, keep):
    copies, rows, _ = arrived.shape
    k = 2 * sums[0].shape[0] // 3
    return pl.pallas_call(
        owner_kernel,
        out_shape=(array((copies, 4 * rows + k, 128), BF), keep((k, 128), F32)),
        in_specs=[VMEM] * 5,
        out_specs=(VMEM, VMEM),
        compiler_params=PARAMS,
    )(arrived, *sums)


def inverse_kernel(totals, out):
    size = 2 * totals.shape[0]
    half = unlanes(totals[...], 2)
    rows = lax.broadcasted_iota(jnp.int32, (size, 2 * size), 0)
    columns = lax.broadcasted_iota(jnp.int32, (size, 2 * size), 1)
    identity = (columns == rows + size).astype(F32)
    work = jnp.concatenate([half, identity[:, size:]], axis=1)
    for j in range(0, size, 2):
        first, second = work[j : j + 1], work[j + 1 : j + 2]
        aa, ab, bb = first[:, j : j + 1], first[:, j + 1 : j + 2], second[:, j + 1 : j + 2]
        scale = 1.0 / (aa * bb - ab * ab)
        top = (bb * scale) * first - (ab * scale) * second
        bottom = (aa * scale) * second - (ab * scale) * first
        rest = work - work[:, j : j + 1] * top - work[:, j + 1 : j + 2] * bottom
        work = jnp.where(rows == j, top, jnp.where(rows == j + 1, bottom, rest))
    out[...] = work[:, size:]


def inverse_of(totals, keep):
    size = 2 * totals.shape[0]
    return pl.pallas_call(
        inverse_kernel,
        out_shape=keep((size, size), F32),
        in_specs=[VMEM],
        out_specs=VMEM,
        compiler_params=PARAMS,
    )(totals)


def solve(pieces, inverse, k, rows):
    tail = jnp.zeros((k, 4 * k), F32)
    for j in range(pieces.shape[0]):
        tail += pieces[j, 4 * rows :, :].astype(F32)
    projected = unlanes(tail[: k // 2] + tail[k // 2 :], 4)
    return dot(inverse[...], projected, NN, HIGHEST)


def fock_rows(pieces, i, k, rows):
    per_row = k // rows
    parts = [lanes(pieces[i * per_row + h, : 4 * rows, :], 4) for h in range(per_row)]
    return jnp.concatenate(parts, axis=0).astype(F32)


def step_kernel(pieces, inverse, own, other, gap, out):
    r, k, _ = own.shape
    rows = (pieces.shape[1] - k) // 4
    high, low = split(solve(pieces, inverse, k, rows))
    high, low = high.astype(BF), low.astype(BF)
    for i in range(r):
        both = jnp.concatenate([own[i], other[i]], axis=0)
        mixed = dot(high, both, TN) + dot(low, both, TN)
        value = (mixed - fock_rows(pieces, i, k, rows)) / gap[i : i + 1, :]
        out[i] = value.astype(BF)


def step_update(pieces, inverse, own, other, gap):
    return pl.pallas_call(
        step_kernel,
        out_shape=array(own.shape, BF),
        in_specs=[VMEM] * 5,
        out_specs=VMEM,
        compiler_params=PARAMS,
    )(pieces, inverse, own, other, gap)


def last_kernel(place, pieces, inverse, own, other, gap, out, coupling):
    r, k, _ = own.shape
    rows = (pieces.shape[1] - k) // 4
    solved = solve(pieces, inverse, k, rows)
    turned = solved.T
    swapped = jnp.concatenate([turned[:, k:], turned[:, :k]], axis=1)
    coupling[...] = jnp.where(place[0] == 0, turned, swapped)
    high, low = split(solved)
    high, low = high.astype(BF), low.astype(BF)
    for i in range(r):
        both = jnp.concatenate([own[i], other[i]], axis=0)
        mixed = dot(high, both, TN) + dot(low, both, TN)
        value = (mixed - fock_rows(pieces, i, k, rows)) / gap[i : i + 1, :]
        out[i] = value


def last_update(place, pieces, inverse, own, other, gap):
    r, k, n = own.shape
    vectors, coupling = pl.pallas_call(
        last_kernel,
        out_shape=(array((r, k, n), F32), array((k, 2 * k), F32)),
        in_specs=[SMEM] + [VMEM] * 5,
        out_specs=(VMEM, VMEM),
        compiler_params=PARAMS,
    )(place, pieces, inverse, own, other, gap)
    return jnp.transpose(vectors, (1, 0, 2)), coupling.T


def ring(step):
    pairs = []
    for h in range(4):
        for c in range(2):
            way = step if c == 1 else -step
            pairs.append((2 * h + c, 2 * ((h + way) % 4) + c))
    return pairs


AHEAD = ring(1)
BACK = ring(-1)
SIBLING = [(i, i ^ 1) for i in range(8)]
OTHER = [(0, 1), (1, 0)]


def in_hbm(value):
    return pltpu.with_memory_space_constraint(value, pltpu.HBM)


def per_device(factors, trial_vectors, energy_gap):
    place = jnp.stack([lax.axis_index(a) for a in ("gx", "gy", "gz")])
    own = jnp.transpose(trial_vectors, (1, 0, 2)).astype(BF)
    b = jnp.transpose(factors, (1, 0, 2))

    for iteration in range(ITERS):
        last = iteration == ITERS - 1
        theirs_far, mine_far = mix(place, own, b, (2,))
        theirs, *mine = mix(place, own, b, (-1, 1, 0))
        theirs_far = lax.ppermute(theirs_far, "gz", SIBLING)
        far = lax.ppermute(add(mine_far, theirs_far, 0), "gz", AHEAD)
        theirs = lax.ppermute(theirs, "gz", SIBLING)
        near = lax.ppermute(add(mine[0], theirs, 0), "gz", BACK)
        far = lax.ppermute(add(mine[1], theirs, 1, far), "gz", AHEAD)
        first = add(mine[2], theirs, 2, near, far)
        second = lax.ppermute(first, "gz", AHEAD)
        paired = lax.ppermute(first, "gz", SIBLING)
        third = lax.ppermute(first, "gz", BACK)
        fourth = lax.ppermute(second, "gz", AHEAD)
        other = lax.ppermute(own, "gx", OTHER)
        blocks = [first, second, third, fourth, paired]
        blocks += [lax.ppermute(a, "gz", SIBLING) for a in blocks[1:4]]
        gram = gram_parts(own, other, energy_gap)
        fock, sums = fock_parts(place, blocks, b, own, other, gram)
        arrived = lax.all_to_all(
            fock.reshape(16, -1, fock.shape[1]), "gy", 0, 0, tiled=True
        )
        sums = sums + lax.ppermute(sums, "gz", SIBLING)
        sums = [sums] + [
            lax.ppermute(sums, "gz", [(i, i ^ flip) for i in range(8)])
            for flip in (2, 4, 6)
        ]
        own, other = in_hbm(own), in_hbm(other)
        keep = array if last else pltpu.HBM
        pieces, totals = owner_sums(arrived, sums, keep)
        pieces = lax.all_to_all(pieces, "gy", 0, 0, tiled=True)
        inverse = inverse_of(totals if last else in_hbm(totals), keep)
        if last:
            return last_update(place, pieces, inverse, own, other, energy_gap)
        own = step_update(in_hbm(pieces), in_hbm(inverse), own, other, energy_gap)


def solution(mesh):
    placed = (P("gy", None, "gz"), P("gx", None, "gz"), P(None, "gz"))
    return jax.shard_map(
        per_device,
        mesh=mesh,
        in_specs=placed,
        out_specs=(P("gx", None, "gz"), P(None, "gx")),
        check_vma=False,
    )
```

```python
import jax
import jax.numpy as jnp
from jax import lax
from jax.experimental import pallas as pl
from jax.experimental.pallas import tpu as pltpu
from jax.sharding import PartitionSpec as P

ITERS = 2
BF = jnp.bfloat16
F32 = jnp.float32
HIGHEST = lax.Precision.HIGHEST


NT = (((1,), (1,)), ((), ()))
NN = (((1,), (0,)), ((), ()))
TN = (((0,), (0,)), ((), ()))


def dot(a, b, dims, precision=None):
    return lax.dot_general(a, b, dims, precision=precision, preferred_element_type=F32)


SMEM = pl.BlockSpec(memory_space=pltpu.SMEM)
VMEM = pl.BlockSpec(memory_space=pltpu.VMEM)
PARAMS = pltpu.CompilerParams(vmem_limit_bytes=24 << 20)


def array(shape, dtype):
    return jax.ShapeDtypeStruct(shape, dtype)


def split(value):
    high = value.astype(BF).astype(F32)
    return high, value - high


def lanes(value, parts):
    rows = value.shape[0] // parts
    return jnp.concatenate([value[i * rows : (i + 1) * rows] for i in range(parts)], axis=1)


def unlanes(value, parts):
    width = value.shape[1] // parts
    return jnp.concatenate([value[:, i * width : (i + 1) * width] for i in range(parts)], axis=0)


def rows_of(steps, place, sibling):
    chip = place >> 1
    core = (1 - (place & 1)) if sibling else (place & 1)
    way = 2 * core - 1
    return [2 * ((chip + s * way) & 3) + core for s in steps]


def mix_kernel(place, x, b, *outs, steps):
    rows = x.shape[1]
    count = len(steps)
    order = rows_of(steps, place[2], True) + rows_of(steps, place[2], False)
    chosen = jnp.concatenate([x[j] for j in order], axis=0)
    for r in range(b.shape[0]):
        part = dot(chosen, b[r], NT)
        for j in range(count):
            theirs = part[j * rows : (j + 1) * rows]
            outs[0][j, r * rows : (r + 1) * rows, :] = theirs.astype(BF)
            mine = part[(count + j) * rows : (count + j + 1) * rows]
            outs[1 + j][r * rows : (r + 1) * rows, :] = mine


def mix(place, x, b, steps):
    r, k, _ = x.shape
    shape = (r * k, b.shape[1])
    outs = [array((len(steps), *shape), BF)] + [array(shape, F32)] * len(steps)
    return pl.pallas_call(
        lambda *refs: mix_kernel(*refs, steps=steps),
        out_shape=outs,
        in_specs=[SMEM, VMEM, VMEM],
        out_specs=[VMEM] * len(outs),
        compiler_params=PARAMS,
    )(place, x, b)


def add_kernel(mine, theirs, *refs):
    *others, out = refs
    total = mine[...] + theirs[0].astype(F32)
    for other in others:
        total += other[...].astype(F32)
    out[...] = total.astype(BF)


def add(mine, theirs, index, *others):
    whole = pl.BlockSpec(mine.shape, lambda i: (0, 0))
    return pl.pallas_call(
        add_kernel,
        grid=(1,),
        out_shape=array(mine.shape, BF),
        in_specs=[whole, pl.BlockSpec((1, *mine.shape), lambda i: (index, 0, 0))]
        + [whole] * len(others),
        out_specs=whole,
        compiler_params=PARAMS,
    )(mine, theirs, *others)


def gram_kernel(own, other, gap, out):
    r, k, _ = own.shape
    gram = jnp.zeros((2 * k, 2 * k), F32)
    scaled = jnp.zeros((2 * k, k), F32)
    for i in range(r):
        both = jnp.concatenate([own[i], other[i]], axis=0)
        gram += dot(both, both, NT)
        high, low = split(own[i].astype(F32) * gap[i : i + 1, :])
        scaled += dot(both, high.astype(BF), NT) + dot(both, low.astype(BF), NT)
    out[...] = jnp.concatenate([gram, scaled], axis=1)


def gram_parts(own, other, gap):
    k = own.shape[1]
    return pl.pallas_call(
        gram_kernel,
        out_shape=array((2 * k, 3 * k), F32),
        in_specs=[VMEM] * 3,
        out_specs=VMEM,
        compiler_params=PARAMS,
    )(own, other, gap)


def fock_kernel(place, *refs):
    blocks = refs[:8]
    b, own, other, gram, out, message, coulomb = refs[8:]
    r, k, _ = own.shape
    rows = r * k
    got = (0, -1, 1, 2)
    order = rows_of(got, place[2], False) + rows_of(got, place[2], True)
    fitted = jnp.zeros((k, blocks[0].shape[1]), F32)
    for j in range(8):
        start = pl.multiple_of(order[j] * k, k)
        fitted += blocks[j][pl.ds(start, k), :].astype(F32)
    fitted = fitted.astype(BF)
    total = jnp.zeros((rows, b.shape[2]), F32)
    for j in range(8):
        both = dot(jnp.concatenate([blocks[j][...], fitted], axis=0), b[order[j]], NN)
        total += both[:rows]
        coulomb[order[j]] = both[rows:]
    projected = jnp.zeros((2 * k, k), F32)
    for i in range(r):
        part = 2.0 * coulomb[i] - total[i * k : (i + 1) * k]
        part = part.astype(BF)
        out[i * k : (i + 1) * k, :] = part
        projected += dot(jnp.concatenate([own[i], other[i]], axis=0), part, NT)
    once = jnp.where(place[1] == 0, 1.0, 0.0)
    projected += once * gram[:, 2 * k :]
    message[...] = jnp.concatenate([lanes(gram[:, : 2 * k], 2), lanes(projected, 4)], axis=0)


def fock_parts(place, blocks, b, own, other, gram):
    r, k, n = own.shape
    return pl.pallas_call(
        fock_kernel,
        out_shape=(array((r * k, n), BF), array((3 * k // 2, 4 * k), F32)),
        in_specs=[SMEM] + [VMEM] * 12,
        out_specs=(VMEM, VMEM),
        scratch_shapes=[pltpu.VMEM((r, k, n), F32)],
        compiler_params=PARAMS,
    )(place, *blocks, b, own, other, gram)


def owner_kernel(arrived, s0, s1, s2, s3, out, totals):
    total = (s0[...] + s1[...]) + (s2[...] + s3[...])
    size = totals.shape[0]
    totals[...] = total[:size]
    high, low = split(total[size:])
    tail = jnp.concatenate([high, low], axis=0).astype(BF)
    fock = arrived[0].astype(F32)
    for j in range(1, arrived.shape[0]):
        fock += arrived[j].astype(F32)
    fock = fock.astype(BF)
    rows = fock.shape[0]
    for p in range(out.shape[0]):
        for i in range(4):
            out[p, i * rows : (i + 1) * rows, :] = fock[:, i * 128 : (i + 1) * 128]
        out[p, 4 * rows :, :] = tail


def owner_sums(arrived, sums, keep):
    copies, rows, _ = arrived.shape
    k = 2 * sums[0].shape[0] // 3
    return pl.pallas_call(
        owner_kernel,
        out_shape=(array((copies, 4 * rows + k, 128), BF), keep((k, 128), F32)),
        in_specs=[VMEM] * 5,
        out_specs=(VMEM, VMEM),
        compiler_params=PARAMS,
    )(arrived, *sums)


def inverse_kernel(totals, out):
    size = 2 * totals.shape[0]
    half = unlanes(totals[...], 2)
    rows = lax.broadcasted_iota(jnp.int32, (size, 2 * size), 0)
    columns = lax.broadcasted_iota(jnp.int32, (size, 2 * size), 1)
    identity = (columns == rows + size).astype(F32)
    work = jnp.concatenate([half, identity[:, size:]], axis=1)
    for j in range(0, size, 2):
        first, second = work[j : j + 1], work[j + 1 : j + 2]
        aa, ab, bb = first[:, j : j + 1], first[:, j + 1 : j + 2], second[:, j + 1 : j + 2]
        scale = 1.0 / (aa * bb - ab * ab)
        top = (bb * scale) * first - (ab * scale) * second
        bottom = (aa * scale) * second - (ab * scale) * first
        rest = work - work[:, j : j + 1] * top - work[:, j + 1 : j + 2] * bottom
        work = jnp.where(rows == j, top, jnp.where(rows == j + 1, bottom, rest))
    out[...] = work[:, size:]


def inverse_of(totals, keep):
    size = 2 * totals.shape[0]
    return pl.pallas_call(
        inverse_kernel,
        out_shape=keep((size, size), F32),
        in_specs=[VMEM],
        out_specs=VMEM,
        compiler_params=PARAMS,
    )(totals)


def solve(pieces, inverse, k, rows):
    tail = jnp.zeros((k, 4 * k), F32)
    for j in range(pieces.shape[0]):
        tail += pieces[j, 4 * rows :, :].astype(F32)
    projected = unlanes(tail[: k // 2] + tail[k // 2 :], 4)
    return dot(inverse[...], projected, NN, HIGHEST)


def fock_rows(pieces, i, k, rows):
    per_row = k // rows
    parts = [lanes(pieces[i * per_row + h, : 4 * rows, :], 4) for h in range(per_row)]
    return jnp.concatenate(parts, axis=0).astype(F32)


def step_kernel(pieces, inverse, own, other, gap, out):
    r, k, _ = own.shape
    rows = (pieces.shape[1] - k) // 4
    high, low = split(solve(pieces, inverse, k, rows))
    high, low = high.astype(BF), low.astype(BF)
    for i in range(r):
        both = jnp.concatenate([own[i], other[i]], axis=0)
        mixed = dot(high, both, TN) + dot(low, both, TN)
        value = (mixed - fock_rows(pieces, i, k, rows)) / gap[i : i + 1, :]
        out[i] = value.astype(BF)


def step_update(pieces, inverse, own, other, gap):
    return pl.pallas_call(
        step_kernel,
        out_shape=array(own.shape, BF),
        in_specs=[VMEM] * 5,
        out_specs=VMEM,
        compiler_params=PARAMS,
    )(pieces, inverse, own, other, gap)


def last_kernel(place, pieces, inverse, own, other, gap, out, coupling):
    r, k, _ = own.shape
    rows = (pieces.shape[1] - k) // 4
    solved = solve(pieces, inverse, k, rows)
    turned = solved.T
    swapped = jnp.concatenate([turned[:, k:], turned[:, :k]], axis=1)
    coupling[...] = jnp.where(place[0] == 0, turned, swapped)
    high, low = split(solved)
    high, low = high.astype(BF), low.astype(BF)
    for i in range(r):
        both = jnp.concatenate([own[i], other[i]], axis=0)
        mixed = dot(high, both, TN) + dot(low, both, TN)
        value = (mixed - fock_rows(pieces, i, k, rows)) / gap[i : i + 1, :]
        out[:, i, :] = value


def last_update(place, pieces, inverse, own, other, gap):
    r, k, n = own.shape
    vectors, coupling = pl.pallas_call(
        last_kernel,
        out_shape=(array((k, r, n), F32), array((k, 2 * k), F32)),
        in_specs=[SMEM] + [VMEM] * 5,
        out_specs=(VMEM, VMEM),
        compiler_params=PARAMS,
    )(place, pieces, inverse, own, other, gap)
    return vectors, coupling.T


def ring(step):
    pairs = []
    for h in range(4):
        for c in range(2):
            way = step if c == 1 else -step
            pairs.append((2 * h + c, 2 * ((h + way) % 4) + c))
    return pairs


AHEAD = ring(1)
BACK = ring(-1)
SIBLING = [(i, i ^ 1) for i in range(8)]
OTHER = [(0, 1), (1, 0)]


def in_hbm(value):
    return pltpu.with_memory_space_constraint(value, pltpu.HBM)


def per_device(factors, trial_vectors, energy_gap):
    place = jnp.stack([lax.axis_index(a) for a in ("gx", "gy", "gz")])
    own = jnp.transpose(trial_vectors, (1, 0, 2)).astype(BF)
    b = jnp.transpose(factors, (1, 0, 2))

    for iteration in range(ITERS):
        last = iteration == ITERS - 1
        theirs_far, mine_far = mix(place, own, b, (2,))
        theirs, *mine = mix(place, own, b, (-1, 1, 0))
        theirs_far = lax.ppermute(theirs_far, "gz", SIBLING)
        far = lax.ppermute(add(mine_far, theirs_far, 0), "gz", AHEAD)
        theirs = lax.ppermute(theirs, "gz", SIBLING)
        near = lax.ppermute(add(mine[0], theirs, 0), "gz", BACK)
        far = lax.ppermute(add(mine[1], theirs, 1, far), "gz", AHEAD)
        first = add(mine[2], theirs, 2, near, far)
        second = lax.ppermute(first, "gz", AHEAD)
        paired = lax.ppermute(first, "gz", SIBLING)
        third = lax.ppermute(first, "gz", BACK)
        fourth = lax.ppermute(second, "gz", AHEAD)
        other = lax.ppermute(own, "gx", OTHER)
        blocks = [first, second, third, fourth, paired]
        blocks += [lax.ppermute(a, "gz", SIBLING) for a in blocks[1:4]]
        gram = gram_parts(own, other, energy_gap)
        fock, sums = fock_parts(place, blocks, b, own, other, gram)
        arrived = lax.all_to_all(
            fock.reshape(16, -1, fock.shape[1]), "gy", 0, 0, tiled=True
        )
        sums = sums + lax.ppermute(sums, "gz", SIBLING)
        sums = [sums] + [
            lax.ppermute(sums, "gz", [(i, i ^ flip) for i in range(8)])
            for flip in (2, 4, 6)
        ]
        own, other = in_hbm(own), in_hbm(other)
        keep = array if last else pltpu.HBM
        pieces, totals = owner_sums(arrived, sums, keep)
        pieces = lax.all_to_all(pieces, "gy", 0, 0, tiled=True)
        inverse = inverse_of(totals if last else in_hbm(totals), keep)
        if last:
            return last_update(place, pieces, inverse, own, other, energy_gap)
        own = step_update(in_hbm(pieces), in_hbm(inverse), own, other, energy_gap)


def solution(mesh):
    placed = (P("gy", None, "gz"), P("gx", None, "gz"), P(None, "gz"))
    return jax.shard_map(
        per_device,
        mesh=mesh,
        in_specs=placed,
        out_specs=(P("gx", None, "gz"), P(None, "gx")),
        check_vma=False,
    )
```
